8 devices in a mesh: case: 2 (over z, y), ens: 4 (over x, core).
Axes of the slice: x: 2, y: 2, z: 1, core: 2. Of those that a mesh axis runs over, the one named last changes fastest.
Arguments:
- x_init: float32 [48, 1024, 128], P(('case', 'ens')), parts along dimension 0
- col_mix: bfloat16 [1024, 1024], replicated
- w_in: bfloat16 [3, 128, 512], replicated
- w_out: bfloat16 [3, 512, 128], replicated
- obs_val: float32 [2, 2048, 4], P(None, ('case', 'ens')), parts along dimension 1
- obs_rinv: float32 [2048, 4], P(('case', 'ens')), parts along dimension 0
- obs_idx: int32 [4], replicated
- inflation: float32 [1], replicated
Outputs:
- output: float32 [48, 1024, 128], P(('case', 'ens')), parts along dimension 0
There are 2 independent parts. The reference program is written for one: setup_inputs(seed, part) draws one part's arguments, and reference() takes and returns one part's arrays. A program takes and returns all parts, laid end to end along the dimension named above; an argument that names none is the same for every part.
All inputs are finite; a program needn't handle non-finite values.
Results may differ from the reference program's by a relative error of at most 0.0130914.
Values are sent between devices in bfloat16 or wider.
A program may use at most 1 GiB of HBM per device.

```python
import math
import jax
import jax.numpy as jnp
from jax import lax

MEMBERS = 24
COLS = 1024
V = 128
FF = 512
OBS = 4
LAYERS = 3
NS_STEPS = 12
CYCLES = 2
COL_BLOCK = math.gcd(COLS, 32)
NBLOCKS = COLS // COL_BLOCK


def setup_inputs(seed: int = 0, part: int = 0) -> dict:
    base_key = jax.random.key(seed)
    shared_keys = jax.random.split(base_key, 5)
    part_keys = jax.random.split(jax.random.fold_in(base_key, part), 4)
    mean_field = jax.random.normal(part_keys[0], (COLS, V), jnp.float32)
    spread = 0.5 * jax.random.normal(part_keys[1], (MEMBERS, COLS, V), jnp.float32)
    col_mix = jax.random.normal(shared_keys[0], (COLS, COLS), jnp.float32) * COLS ** -0.5
    w_in = jax.random.normal(shared_keys[1], (LAYERS, V, FF), jnp.float32) * V ** -0.5
    w_out = 0.7 * jax.random.normal(shared_keys[2], (LAYERS, FF, V), jnp.float32) * FF ** -0.5
    return {
        'x_init': mean_field[None] + spread,
        'col_mix': col_mix.astype(jnp.bfloat16),
        'w_in': w_in.astype(jnp.bfloat16),
        'w_out': w_out.astype(jnp.bfloat16),
        'obs_val': jax.random.normal(part_keys[2], (CYCLES, COLS, OBS), jnp.float32),
        'obs_rinv': jax.random.uniform(part_keys[3], (COLS, OBS), jnp.float32, 1.0, 6.0),
        'obs_idx': jax.random.permutation(shared_keys[3], V)[:OBS].astype(jnp.int32),
        'inflation': jax.random.uniform(shared_keys[4], (1,), jnp.float32, 1.1, 1.6),
    }


def forecast_member(member, col_mix, w_in, w_out):
    def layer_step(hid_state, weights):
        w_first, w_second = weights
        mixed_cols = jnp.dot(col_mix, hid_state.astype(jnp.bfloat16), preferred_element_type=jnp.float32).astype(jnp.bfloat16)
        hidden = jax.nn.gelu(jnp.dot(mixed_cols, w_first, preferred_element_type=jnp.float32), approximate=True).astype(jnp.bfloat16)
        return hid_state + jnp.dot(hidden, w_second, preferred_element_type=jnp.float32), None
    result, _ = lax.scan(layer_step, member, (w_in, w_out))
    return result


def analyse(ens_blk, obs_now, rinv_now, obs_idx, inflation):
    ens_mean = jnp.mean(ens_blk, axis=0)
    ens_pert = ens_blk - ens_mean
    obs_pert = jnp.take(ens_pert, obs_idx, axis=2)
    innovation = obs_now - jnp.take(ens_mean, obs_idx, axis=1)
    gain_in = obs_pert * rinv_now
    ident = jnp.eye(MEMBERS, dtype=jnp.float32)
    a_mat = ((MEMBERS - 1) / inflation[0]) * ident + jnp.einsum('kbp,lbp->bkl', gain_in, obs_pert)
    fro_norm = jnp.sqrt(jnp.sum(a_mat * a_mat, axis=(1, 2)))

    def ns_step(ns_pair, _):
        r_iter, z_iter = ns_pair
        t_mat = 1.5 * ident - 0.5 * jnp.einsum('bij,bjk->bik', z_iter, r_iter)
        return (jnp.einsum('bij,bjk->bik', r_iter, t_mat), jnp.einsum('bij,bjk->bik', t_mat, z_iter)), None

    init_pair = (a_mat / fro_norm[:, None, None], jnp.broadcast_to(ident, a_mat.shape))
    (_, z_last), _ = lax.scan(ns_step, init_pair, None, length=NS_STEPS)
    s_mat = z_last / jnp.sqrt(fro_norm)[:, None, None]
    gain_vec = jnp.einsum('kbp,bp->bk', gain_in, innovation)
    w_mean = jnp.einsum('bij,bj->bi', s_mat, jnp.einsum('bij,bj->bi', s_mat, gain_vec))
    w_full = math.sqrt(MEMBERS - 1) * s_mat + w_mean[:, :, None]
    return ens_mean + jnp.einsum('bik,ibv->kbv', w_full, ens_pert)


def reference(x_init, col_mix, w_in, w_out, obs_val, obs_rinv, obs_idx, inflation):
    rinv_blocks = obs_rinv.reshape(NBLOCKS, COL_BLOCK, OBS)

    def cycle_step(ens_state, obs_now):
        forecast = lax.map(lambda member: forecast_member(member, col_mix, w_in, w_out), ens_state)
        col_blocks = forecast.reshape(MEMBERS, NBLOCKS, COL_BLOCK, V).transpose(1, 0, 2, 3)
        obs_blocks = obs_now.reshape(NBLOCKS, COL_BLOCK, OBS)
        analysed = lax.map(lambda block_args: analyse(block_args[0], block_args[1], block_args[2], obs_idx, inflation), (col_blocks, obs_blocks, rinv_blocks))
        return analysed.transpose(1, 0, 2, 3).reshape(MEMBERS, COLS, V), None

    final_state, _ = lax.scan(cycle_step, x_init, obs_val)
    return final_state
```

```python
import math
import jax
import jax.numpy as jnp
from jax import lax
from jax.sharding import PartitionSpec as P

NS_STEPS = 12
OBS = 4
PAIRS = [(p, q) for p in range(OBS) for q in range(p, OBS)]


def sym(p, q):
    return (p, q) if p <= q else (q, p)


def smul(a, b):
    return {(p, q): sum(a[sym(p, t)] * b[sym(t, q)] for t in range(OBS)) for p, q in PAIRS}


def shift(c, a):
    return {pq: (v + c if pq[0] == pq[1] else v) for pq, v in a.items()}


def scale_add(x, a, y, b):
    return {pq: x * a[pq] + y * b[pq] for pq in a}


def ns_weights(cov, rinv, innov, inflation, members):
    root_r = [jnp.sqrt(r) for r in rinv]
    c_mat = {(p, q): cov[(p, q)] * root_r[p] * root_r[q] for p, q in PAIRS}
    base = (members - 1) / inflation
    hat = shift(base, c_mat)
    norm2 = (members - OBS) * base * base
    for (p, q), v in hat.items():
        norm2 = norm2 + (v * v if p == q else 2.0 * (v * v))
    norm = jnp.sqrt(norm2)
    inv = 1.0 / norm
    rho, r_low, r_hat = base * inv, None, {pq: v * inv for pq, v in hat.items()}
    zero = jnp.zeros_like(inv)
    r_low = {pq: (inv if pq[0] == pq[1] else zero) for pq in PAIRS}
    zeta, z_low = jnp.ones_like(inv), {pq: zero for pq in PAIRS}
    for _ in range(NS_STEPS):
        prod = smul(z_low, r_hat)
        t_low = {pq: -0.5 * (zeta * r_low[pq] + prod[pq]) for pq in PAIRS}
        tau = 1.5 - 0.5 * (zeta * rho)
        t_hat = shift(tau, smul(c_mat, t_low))
        pr, pz = smul(r_low, t_hat), smul(z_low, t_hat)
        r_low = {pq: rho * t_low[pq] + pr[pq] for pq in PAIRS}
        z_low = {pq: zeta * t_low[pq] + pz[pq] for pq in PAIRS}
        rho, zeta = rho * tau, zeta * tau
        r_hat = shift(rho, smul(c_mat, r_low))
    inv_root = 1.0 / jnp.sqrt(norm)
    zs = zeta * inv_root
    q_mat = {pq: v * inv_root for pq, v in z_low.items()}
    s_hat = shift(zs, smul(c_mat, q_mat))
    vec = [root_r[p] * innov[p] for p in range(OBS)]
    for _ in range(2):
        vec = [sum(s_hat[sym(p, q)] * vec[q] for q in range(OBS)) for p in range(OBS)]
    fac = math.sqrt(members - 1)
    a = fac * zs
    g = {(p, q): fac * root_r[p] * root_r[q] * q_mat[(p, q)] for p, q in PAIRS}
    e = [root_r[p] * vec[p] for p in range(OBS)]
    return a, g, e


def value_a8(ens_state, col_mix, w_in, w_out):
    for layer_idx in range(w_in.shape[0]):
        mixed_cols = jnp.einsum('ij,...jv->...iv', col_mix, ens_state.astype(jnp.bfloat16), preferred_element_type=jnp.float32).astype(jnp.bfloat16)
        hidden = jax.nn.gelu(jnp.einsum('...v,vf->...f', mixed_cols, w_in[layer_idx], preferred_element_type=jnp.float32), approximate=True).astype(jnp.bfloat16)
        ens_state = ens_state + jnp.einsum('...f,fv->...v', hidden, w_out[layer_idx], preferred_element_type=jnp.float32)
    return ens_state


def analyse(ens_blk, obs_now, rinv_now, obs_idx, inflation):
    members = ens_blk.shape[0]
    ens_mean = jnp.mean(ens_blk, axis=0)
    ens_pert = ens_blk - ens_mean
    obs_pert = jnp.take(ens_pert, obs_idx, axis=2)
    innovation = obs_now - jnp.take(ens_mean, obs_idx, axis=1)
    moments = [jnp.sum(obs_pert[:, :, p:p + 1] * ens_pert, axis=0) for p in range(OBS)]
    cov = {(p, q): jnp.sum(obs_pert[:, :, p] * obs_pert[:, :, q], axis=0) for p, q in PAIRS}
    a, g, e = ns_weights(cov, [rinv_now[:, p] for p in range(OBS)], [innovation[:, p] for p in range(OBS)], inflation[0], members)
    new_mean = ens_mean + sum(e[p][:, None] * moments[p] for p in range(OBS))
    mixed = [sum(g[sym(p, q)][:, None] * moments[q] for q in range(OBS)) for p in range(OBS)]
    out = new_mean + a[:, None] * ens_pert
    for p in range(OBS):
        out = out + obs_pert[:, :, p:p + 1] * mixed[p]
    return out


def solution(mesh):
    def per_device(x_loc, col_mix, w_in, w_out, obs_loc, rinv_loc, obs_idx, inflation):
        ens_state = x_loc
        for cycle_idx in range(obs_loc.shape[0]):
            ens_state = value_a8(ens_state, col_mix, w_in, w_out)
            by_column = lax.all_to_all(ens_state, 'ens', 1, 0, tiled=True)
            analysed = analyse(by_column, obs_loc[cycle_idx], rinv_loc, obs_idx, inflation)
            ens_state = lax.all_to_all(analysed, 'ens', 0, 1, tiled=True)
        return ens_state

    state_spec = P(('case', 'ens'), None, None)
    in_specs = (state_spec, P(), P(), P(), P(None, ('case', 'ens'), None), P(('case', 'ens'), None), P(), P())
    return jax.shard_map(per_device, mesh=mesh, in_specs=in_specs, out_specs=state_spec, check_vma=False)
```

```python
import functools
import math
import jax
import jax.numpy as jnp
from jax import lax
from jax.experimental import pallas as pl
from jax.experimental.pallas import tpu as pltpu
from jax.sharding import PartitionSpec as P

NS_STEPS = 12
OBS = 4
PAIRS = [(p, q) for p in range(OBS) for q in range(p, OBS)]


def sym(p, q):
    return (p, q) if p <= q else (q, p)


def smul(a, b):
    return {(p, q): sum(a[sym(p, t)] * b[sym(t, q)] for t in range(OBS)) for p, q in PAIRS}


def shift(c, a):
    return {pq: (v + c if pq[0] == pq[1] else v) for pq, v in a.items()}


def scale_add(x, a, y, b):
    return {pq: x * a[pq] + y * b[pq] for pq in a}


def ns_weights(cov, rinv, innov, inflation, members):
    root_r = [jnp.sqrt(r) for r in rinv]
    c_mat = {(p, q): cov[(p, q)] * root_r[p] * root_r[q] for p, q in PAIRS}
    base = (members - 1) / inflation
    hat = shift(base, c_mat)
    norm2 = (members - OBS) * base * base
    for (p, q), v in hat.items():
        norm2 = norm2 + (v * v if p == q else 2.0 * (v * v))
    norm = jnp.sqrt(norm2)
    inv = 1.0 / norm
    rho, r_low, r_hat = base * inv, None, {pq: v * inv for pq, v in hat.items()}
    zero = jnp.zeros_like(inv)
    r_low = {pq: (inv if pq[0] == pq[1] else zero) for pq in PAIRS}
    zeta, z_low = jnp.ones_like(inv), {pq: zero for pq in PAIRS}
    for _ in range(NS_STEPS):
        prod = smul(z_low, r_hat)
        t_low = {pq: -0.5 * (zeta * r_low[pq] + prod[pq]) for pq in PAIRS}
        tau = 1.5 - 0.5 * (zeta * rho)
        t_hat = shift(tau, smul(c_mat, t_low))
        pr, pz = smul(r_low, t_hat), smul(z_low, t_hat)
        r_low = {pq: rho * t_low[pq] + pr[pq] for pq in PAIRS}
        z_low = {pq: zeta * t_low[pq] + pz[pq] for pq in PAIRS}
        rho, zeta = rho * tau, zeta * tau
        r_hat = shift(rho, smul(c_mat, r_low))
    inv_root = 1.0 / jnp.sqrt(norm)
    zs = zeta * inv_root
    q_mat = {pq: v * inv_root for pq, v in z_low.items()}
    s_hat = shift(zs, smul(c_mat, q_mat))
    vec = [root_r[p] * innov[p] for p in range(OBS)]
    for _ in range(2):
        vec = [sum(s_hat[sym(p, q)] * vec[q] for q in range(OBS)) for p in range(OBS)]
    fac = math.sqrt(members - 1)
    a = fac * zs
    g = {(p, q): fac * root_r[p] * root_r[q] * q_mat[(p, q)] for p, q in PAIRS}
    e = [root_r[p] * vec[p] for p in range(OBS)]
    return a, g, e


MESH = pl.DeviceIdType.MESH
CHUNK = 256
BLK = 128
ROWS_O = 5 * BLK
ROWS_C = ROWS_O + OBS
PACK = ROWS_O + 16
VB = 16


def gelu(x):
    u = x * (0.7978845608028654 + 0.035677408136300125 * (x * x))
    y = 0.5 * x
    return y + y * jnp.tanh(u)


def kernel(n_dev, n_layers, n_cycles, members, x_ref, a_ref, w_ref, u_ref, obs_ref, idx_ref, infl_ref, out_ref,
           at, wt, ut, ht, hb, mt, obs_all, part, got_sib, chip, got_chip, tot, coef, yrow,
           obs_send, obs_recv, sib_send, sib_recv, chip_send, chip_recv, tot_send, tot_recv):
    loc_members = x_ref.shape[0]
    cols, nv = x_ref.shape[1], x_ref.shape[2]
    n_chunks = cols // CHUNK
    me = lax.axis_index('ens')
    core = lax.rem(me, 2)
    sib = me + 1 - 2 * core
    mate = lax.rem(me + 2, n_dev)
    obs_i = [idx_ref[p] for p in range(OBS)]

    barrier = pltpu.get_barrier_semaphore()
    for step in range(1, n_dev):
        pl.semaphore_signal(barrier, inc=1, device_id={'ens': lax.rem(me + step, n_dev)}, device_id_type=MESH)
    pl.semaphore_wait(barrier, n_dev - 1)

    def obs_copy(step):
        return pltpu.make_async_remote_copy(
            src_ref=obs_ref, dst_ref=obs_all.at[me], send_sem=obs_send.at[step - 1], recv_sem=obs_recv.at[step - 1],
            device_id={'ens': lax.rem(me + step, n_dev)}, device_id_type=MESH)

    for step in range(1, n_dev):
        obs_copy(step).start()
    obs_all[me] = obs_ref[...]

    def turn(t, _):
        off = pl.multiple_of(t * CHUNK, CHUNK)
        at[t] = a_ref[pl.ds(off, CHUNK), :].T
        for k in range(loc_members):
            blk = x_ref[k, pl.ds(off, CHUNK), :].T
            for b in range(2):
                ht[t, b, k * nv:(k + 1) * nv, :] = blk[:, b * BLK:(b + 1) * BLK]
            hb[0, k * nv:(k + 1) * nv, pl.ds(off, CHUNK)] = blk.astype(jnp.bfloat16)
        return 0
    lax.fori_loop(0, n_chunks, turn, 0)
    for l in range(n_layers):
        wt[l] = w_ref[l].T
        ut[l] = u_ref[l].T

    def layer_chunk(l, t, src, keep):
        off = pl.multiple_of(t * CHUNK, CHUNK)
        mt[...] = jnp.dot(hb[src], at[t], preferred_element_type=jnp.float32).astype(jnp.bfloat16)
        for k in range(loc_members):
            rows = slice(k * nv, (k + 1) * nv)
            hid = gelu(jnp.dot(wt[l], mt[rows, :], preferred_element_type=jnp.float32)).astype(jnp.bfloat16)
            delta = jnp.dot(ut[l], hid, preferred_element_type=jnp.float32)
            for b in range(2):
                new = ht[t, b, rows, :] + delta[:, b * BLK:(b + 1) * BLK]
                ht[t, b, rows, :] = new
                if keep:
                    hb[1 - src, rows, pl.ds(pl.multiple_of(off + b * BLK, BLK), BLK)] = new.astype(jnp.bfloat16)

    def stats(c, t):
        for b in range(2):
            ho = [[ht[t, b, pl.ds(k * nv + obs_i[p], 1), :] for k in range(loc_members)] for p in range(OBS)]
            mo = [sum(h[1:], h[0]) * (1.0 / loc_members) for h in ho]
            y = [[h - mo[p] for h in ho[p]] for p in range(OBS)]
            for p in range(OBS):
                part[c, t, b, ROWS_O + p:ROWS_O + p + 1, :] = mo[p]
            for n, (p, q) in enumerate(PAIRS):
                part[c, t, b, ROWS_C + n:ROWS_C + n + 1, :] = sum(y[p][k] * y[q][k] for k in range(loc_members))
            for v in range(0, nv, VB):
                h = [ht[t, b, k * nv + v:k * nv + v + VB, :] for k in range(loc_members)]
                m = sum(h[1:], h[0]) * (1.0 / loc_members)
                d = [x - m for x in h]
                part[c, t, b, v:v + VB, :] = m
                for p in range(OBS):
                    o = (p + 1) * BLK + v
                    part[c, t, b, o:o + VB, :] = sum(y[p][k] * d[k] for k in range(loc_members))

    def merge(dst, one, two, half_n):
        da = [two[ROWS_O + p:ROWS_O + p + 1, :] - one[ROWS_O + p:ROWS_O + p + 1, :] for p in range(OBS)]
        for p in range(OBS):
            r = ROWS_O + p
            dst[r:r + 1, :] = 0.5 * (one[r:r + 1, :] + two[r:r + 1, :])
        for n, (p, q) in enumerate(PAIRS):
            r = ROWS_C + n
            dst[r:r + 1, :] = one[r:r + 1, :] + two[r:r + 1, :] + (half_n * da[p]) * da[q]
        sc = [half_n * x for x in da]
        for v in range(0, nv, VB):
            ma, mb = one[v:v + VB, :], two[v:v + VB, :]
            dst[v:v + VB, :] = 0.5 * (ma + mb)
            dm = mb - ma
            for p in range(OBS):
                o = (p + 1) * BLK + v
                dst[o:o + VB, :] = one[o:o + VB, :] + two[o:o + VB, :] + sc[p] * dm

    def sib_copy(c, t):
        return pltpu.make_async_remote_copy(
            src_ref=part.at[c, t, 1 - core], dst_ref=got_sib.at[c, t], send_sem=sib_send.at[c, t], recv_sem=sib_recv.at[c, t],
            device_id={'ens': sib}, device_id_type=MESH)

    def chip_copy(c, t):
        return pltpu.make_async_remote_copy(
            src_ref=chip.at[c, t], dst_ref=got_chip.at[c, t], send_sem=chip_send.at[c, t], recv_sem=chip_recv.at[c, t],
            device_id={'ens': mate}, device_id_type=MESH)

    def tot_copy(c, t):
        return pltpu.make_async_remote_copy(
            src_ref=tot.at[c, t, core], dst_ref=tot.at[c, t, core], send_sem=tot_send.at[c, t], recv_sem=tot_recv.at[c, t],
            device_id={'ens': sib}, device_id_type=MESH)

    def first_merge(c, t):
        sib_copy(c, t).wait_recv()
        merge(chip.at[c, t], part.at[c, t, core], got_sib.at[c, t], loc_members / 2)
        chip_copy(c, t).start()

    def second_merge(c, t):
        chip_copy(c, t).wait_recv()
        merge(tot.at[c, t, core], chip.at[c, t], got_chip.at[c, t], loc_members)
        tot_copy(c, t).start()

    def update(c, t):
        off = pl.multiple_of(t * CHUNK, CHUNK)
        tot_copy(c, t).wait_recv()

        def pair(r):
            return jnp.concatenate([tot[c, t, b, r:r + 1, :] for b in range(2)], axis=0)

        def obs_pair(r):
            return jnp.concatenate([obs_all[t, b, pl.ds(r, 1), :] for b in range(2)], axis=0)

        cov = {pq: pair(ROWS_C + n) for n, pq in enumerate(PAIRS)}
        rinv = [obs_pair(p) for p in range(OBS)]
        innov = [obs_pair(OBS * (c + 1) + p) - pair(ROWS_O + p) for p in range(OBS)]
        a, g, e = ns_weights(cov, rinv, innov, infl_ref[0], members)
        coef[0] = a
        for p in range(OBS):
            coef[1 + p] = e[p]
        for n, pq in enumerate(PAIRS):
            coef[1 + OBS + n] = g[pq]
        for b in range(2):
            for k in range(loc_members):
                for p in range(OBS):
                    yrow[b, k * OBS + p] = ht[t, b, pl.ds(k * nv + obs_i[p], 1), :] - tot[c, t, b, ROWS_O + p:ROWS_O + p + 1, :]
            ca = coef[0, b:b + 1, :]
            ce = [coef[1 + p, b:b + 1, :] for p in range(OBS)]
            cg = {pq: coef[1 + OBS + n, b:b + 1, :] for n, pq in enumerate(PAIRS)}
            for v in range(0, nv, VB):
                m = tot[c, t, b, v:v + VB, :]
                mom = [tot[c, t, b, (p + 1) * BLK + v:(p + 1) * BLK + v + VB, :] for p in range(OBS)]
                base = m + sum(ce[p] * mom[p] for p in range(OBS))
                mix = [sum(cg[sym(p, q)] * mom[q] for q in range(OBS)) for p in range(OBS)]
                for k in range(loc_members):
                    r = k * nv + v
                    new = base + ca * (ht[t, b, r:r + VB, :] - m)
                    for p in range(OBS):
                        new = new + yrow[b, k * OBS + p] * mix[p]
                    ht[t, b, r:r + VB, :] = new
                    hb[0, r:r + VB, pl.ds(pl.multiple_of(off + b * BLK, BLK), BLK)] = new.astype(jnp.bfloat16)

    def cycle(c, _):
        for l in range(n_layers - 1):
            def full(t, _, l=l):
                layer_chunk(l, t, l % 2, True)
                return 0
            lax.fori_loop(0, n_chunks, full, 0)

        def last(t, _):
            layer_chunk(n_layers - 1, t, (n_layers - 1) % 2, False)
            stats(c, t)
            sib_copy(c, t).start()

            @pl.when(t > 0)
            def _():
                first_merge(c, t - 1)
            return 0
        lax.fori_loop(0, n_chunks, last, 0)
        first_merge(c, n_chunks - 1)

        @pl.when(c == 0)
        def _():
            for step in range(1, n_dev):
                obs_copy(step).wait()

        def finish(t, _):
            second_merge(c, t)
            update(c, t)
            return 0
        lax.fori_loop(0, n_chunks, finish, 0)

        def drain(t, _):
            sib_copy(c, t).wait_send()
            chip_copy(c, t).wait_send()
            tot_copy(c, t).wait_send()
            return 0
        lax.fori_loop(0, n_chunks, drain, 0)
        return 0
    lax.fori_loop(0, n_cycles, cycle, 0)

    def back(t, _):
        off = pl.multiple_of(t * CHUNK, CHUNK)
        for k in range(loc_members):
            for b in range(2):
                out_ref[k, pl.ds(pl.multiple_of(off + b * BLK, BLK), BLK), :] = ht[t, b, k * nv:(k + 1) * nv, :].T
        return 0
    lax.fori_loop(0, n_chunks, back, 0)


def solution(mesh):
    n_dev = mesh.shape['ens']

    def per_device(x_loc, col_mix, w_in, w_out, obs_loc, rinv_loc, obs_idx, inflation):
        loc, cols, nv = x_loc.shape
        layers, _, ff = w_in.shape
        cycles = obs_loc.shape[0]
        n_chunks = cols // CHUNK
        obs_pack = jnp.concatenate([rinv_loc.T] + [obs_loc[c].T for c in range(cycles)] + [jnp.zeros((OBS, rinv_loc.shape[0]), jnp.float32)], axis=0)
        obs_pack = jnp.stack([obs_pack[:, :BLK], obs_pack[:, BLK:]])
        vm = pl.BlockSpec(memory_space=pltpu.VMEM)
        sm = pl.BlockSpec(memory_space=pltpu.SMEM)
        dma = pltpu.SemaphoreType.DMA
        packet = (PACK, BLK)
        return pl.pallas_call(
            functools.partial(kernel, n_dev, layers, cycles, loc * n_dev),
            out_shape=jax.ShapeDtypeStruct(x_loc.shape, x_loc.dtype),
            in_specs=[vm] * 5 + [sm] * 2,
            out_specs=vm,
            scratch_shapes=[
                pltpu.VMEM((n_chunks, cols, CHUNK), jnp.bfloat16),
                pltpu.VMEM((layers, ff, nv), jnp.bfloat16),
                pltpu.VMEM((layers, nv, ff), jnp.bfloat16),
                pltpu.VMEM((n_chunks, 2, loc * nv, BLK), jnp.float32),
                pltpu.VMEM((2, loc * nv, cols), jnp.bfloat16),
                pltpu.VMEM((loc * nv, CHUNK), jnp.bfloat16),
                pltpu.VMEM((n_dev,) + obs_pack.shape, jnp.float32),
                pltpu.VMEM((cycles, n_chunks, 2) + packet, jnp.float32),
                pltpu.VMEM((cycles, n_chunks) + packet, jnp.float32),
                pltpu.VMEM((cycles, n_chunks) + packet, jnp.float32),
                pltpu.VMEM((cycles, n_chunks) + packet, jnp.float32),
                pltpu.VMEM((cycles, n_chunks, 2) + packet, jnp.float32),
                pltpu.VMEM((16, 2, BLK), jnp.float32),
                pltpu.VMEM((2, loc * OBS, 1, BLK), jnp.float32),
                dma((n_dev - 1,)), dma((n_dev - 1,)),
                dma((cycles, n_chunks)), dma((cycles, n_chunks)),
                dma((cycles, n_chunks)), dma((cycles, n_chunks)),
                dma((cycles, n_chunks)), dma((cycles, n_chunks)),
            ],
            compiler_params=pltpu.CompilerParams(collective_id=0, has_side_effects=True, vmem_limit_bytes=62 * 1024 * 1024),
        )(x_loc, col_mix, w_in, w_out, obs_pack, obs_idx, inflation)

    state_spec = P(('case', 'ens'), None, None)
    in_specs = (state_spec, P(), P(), P(), P(None, ('case', 'ens'), None), P(('case', 'ens'), None), P(), P())
    return jax.shard_map(per_device, mesh=mesh, in_specs=in_specs, out_specs=state_spec, check_vma=False)
```

```python
import functools
import math
import jax
import jax.numpy as jnp
from jax import lax
from jax.experimental import pallas as pl
from jax.experimental.pallas import tpu as pltpu
from jax.sharding import PartitionSpec as P

NS_STEPS = 12
OBS = 4
PAIRS = [(p, q) for p in range(OBS) for q in range(p, OBS)]


def sym(p, q):
    return (p, q) if p <= q else (q, p)


def smul(a, b):
    return {(p, q): sum(a[sym(p, t)] * b[sym(t, q)] for t in range(OBS)) for p, q in PAIRS}


def shift(c, a):
    return {pq: (v + c if pq[0] == pq[1] else v) for pq, v in a.items()}


def scale_add(x, a, y, b):
    return {pq: x * a[pq] + y * b[pq] for pq in a}


def ns_weights(cov, rinv, innov, inflation, members):
    root_r = [jnp.sqrt(r) for r in rinv]
    c_mat = {(p, q): cov[(p, q)] * root_r[p] * root_r[q] for p, q in PAIRS}
    base = (members - 1) / inflation
    hat = shift(base, c_mat)
    norm2 = (members - OBS) * base * base
    for (p, q), v in hat.items():
        norm2 = norm2 + (v * v if p == q else 2.0 * (v * v))
    norm = jnp.sqrt(norm2)
    inv = 1.0 / norm
    rho, r_low, r_hat = base * inv, None, {pq: v * inv for pq, v in hat.items()}
    zero = jnp.zeros_like(inv)
    r_low = {pq: (inv if pq[0] == pq[1] else zero) for pq in PAIRS}
    zeta, z_low = jnp.ones_like(inv), {pq: zero for pq in PAIRS}
    for _ in range(NS_STEPS):
        prod = smul(z_low, r_hat)
        t_low = {pq: -0.5 * (zeta * r_low[pq] + prod[pq]) for pq in PAIRS}
        tau = 1.5 - 0.5 * (zeta * rho)
        t_hat = shift(tau, smul(c_mat, t_low))
        pr, pz = smul(r_low, t_hat), smul(z_low, t_hat)
        r_low = {pq: rho * t_low[pq] + pr[pq] for pq in PAIRS}
        z_low = {pq: zeta * t_low[pq] + pz[pq] for pq in PAIRS}
        rho, zeta = rho * tau, zeta * tau
        r_hat = shift(rho, smul(c_mat, r_low))
    inv_root = 1.0 / jnp.sqrt(norm)
    zs = zeta * inv_root
    q_mat = {pq: v * inv_root for pq, v in z_low.items()}
    s_hat = shift(zs, smul(c_mat, q_mat))
    vec = [root_r[p] * innov[p] for p in range(OBS)]
    for _ in range(2):
        vec = [sum(s_hat[sym(p, q)] * vec[q] for q in range(OBS)) for p in range(OBS)]
    fac = math.sqrt(members - 1)
    a = fac * zs
    g = {(p, q): fac * root_r[p] * root_r[q] * q_mat[(p, q)] for p, q in PAIRS}
    e = [root_r[p] * vec[p] for p in range(OBS)]
    return a, g, e


MESH = pl.DeviceIdType.MESH
CHUNK = 256
WIDE = 512
BLK = 128
ROWS_O = 5 * BLK
ROWS_C = ROWS_O + OBS
PACK = ROWS_O + 16
VB = 16
BF16 = jnp.bfloat16


def dot(a, b):
    return jnp.dot(a, b, preferred_element_type=jnp.float32)


def gelu_of_half(z):
    return z + z * jnp.tanh(z * (2 * 0.7978845608028654 + (8 * 0.035677408136300125) * (z * z)))


def kernel(n_dev, n_cycles, members, x_hbm, a_hbm, w_hbm, u_hbm, rinv_ref, obs_ref, idx_ref, infl_ref, out_hbm,
           av, wv, uv, h, hb, ht, mb, hid, rinv_all, obs_all, part, got_sib, chip, got_chip, tot, coef, yrow,
           load_sem, out_sem, obs_send, obs_recv, sib_send, sib_recv, chip_send, chip_recv, tot_send, tot_recv):
    loc_members, cols, nv = h.shape
    n_layers = wv.shape[0]
    n_chunks = cols // CHUNK
    me = lax.axis_index('ens')
    core = lax.rem(me, 2)
    sib = me + 1 - 2 * core
    mate = lax.rem(me + 2, n_dev)
    obs_i = [idx_ref[p] for p in range(OBS)]

    loads = [pltpu.make_async_copy(src, dst, load_sem.at[i]) for i, (src, dst) in enumerate(((x_hbm, h), (a_hbm, av), (w_hbm, wv), (u_hbm, uv)))]
    for load in loads:
        load.start()

    barrier = pltpu.get_barrier_semaphore()
    for step in range(1, n_dev):
        pl.semaphore_signal(barrier, inc=1, device_id={'ens': lax.rem(me + step, n_dev)}, device_id_type=MESH)
    pl.semaphore_wait(barrier, n_dev - 1)

    def obs_copies(step):
        dev = {'ens': lax.rem(me + step, n_dev)}
        return [pltpu.make_async_remote_copy(src_ref=src, dst_ref=dst.at[me], send_sem=obs_send.at[step - 1, i], recv_sem=obs_recv.at[step - 1, i],
                                             device_id=dev, device_id_type=MESH)
                for i, (src, dst) in enumerate(((rinv_ref, rinv_all), (obs_ref, obs_all)))]

    for step in range(1, n_dev):
        for copy in obs_copies(step):
            copy.start()
    rinv_all[me] = rinv_ref[...]
    obs_all[me] = obs_ref[...]

    loads[0].wait()
    for k in range(loc_members):
        hb[0, :, k * nv:(k + 1) * nv] = h[k].astype(BF16)
    loads[2].wait()
    wv[...] = wv[...] * jnp.bfloat16(0.5)
    loads[3].wait()
    loads[1].wait()

    def layer_rows(l, t, rows, src, last):
        off = pl.multiple_of(t * rows, rows)
        mb[0:rows, :] = dot(av[pl.ds(off, rows), :], hb[src]).astype(BF16)
        for s in range(loc_members + 1):
            if s < loc_members:
                pre = dot(mb[0:rows, s * nv:(s + 1) * nv], wv[l])
            if s >= 1:
                k = s - 1
                new = h[k, pl.ds(off, rows), :] + dot(hid[k % 2, 0:rows, :], uv[l])
                if last:
                    for b in range(2):
                        ht[t, b, k * nv:(k + 1) * nv, :] = new[b * BLK:(b + 1) * BLK, :].T
                else:
                    h[k, pl.ds(off, rows), :] = new
                    hb[1 - src, pl.ds(off, rows), k * nv:(k + 1) * nv] = new.astype(BF16)
            if s < loc_members:
                hid[s % 2, 0:rows, :] = gelu_of_half(pre).astype(BF16)

    def stats(c, t):
        for b in range(2):
            ho = [[ht[t, b, pl.ds(k * nv + obs_i[p], 1), :] for k in range(loc_members)] for p in range(OBS)]
            mo = [sum(x[1:], x[0]) * (1.0 / loc_members) for x in ho]
            y = [[x - mo[p] for x in ho[p]] for p in range(OBS)]
            for p in range(OBS):
                part[c, t, b, ROWS_O + p:ROWS_O + p + 1, :] = mo[p]
            for n, (p, q) in enumerate(PAIRS):
                part[c, t, b, ROWS_C + n:ROWS_C + n + 1, :] = sum(y[p][k] * y[q][k] for k in range(loc_members))
            for v in range(0, nv, VB):
                x = [ht[t, b, k * nv + v:k * nv + v + VB, :] for k in range(loc_members)]
                m = sum(x[1:], x[0]) * (1.0 / loc_members)
                d = [z - m for z in x]
                part[c, t, b, v:v + VB, :] = m
                for p in range(OBS):
                    o = (p + 1) * BLK + v
                    part[c, t, b, o:o + VB, :] = sum(y[p][k] * d[k] for k in range(loc_members))

    def merge(dst, one, two, half_n):
        da = [two[ROWS_O + p:ROWS_O + p + 1, :] - one[ROWS_O + p:ROWS_O + p + 1, :] for p in range(OBS)]
        for p in range(OBS):
            r = ROWS_O + p
            dst[r:r + 1, :] = 0.5 * (one[r:r + 1, :] + two[r:r + 1, :])
        for n, (p, q) in enumerate(PAIRS):
            r = ROWS_C + n
            dst[r:r + 1, :] = one[r:r + 1, :] + two[r:r + 1, :] + (half_n * da[p]) * da[q]
        sc = [half_n * x for x in da]
        for v in range(0, nv, VB):
            ma, mbb = one[v:v + VB, :], two[v:v + VB, :]
            dst[v:v + VB, :] = 0.5 * (ma + mbb)
            dm = mbb - ma
            for p in range(OBS):
                o = (p + 1) * BLK + v
                dst[o:o + VB, :] = one[o:o + VB, :] + two[o:o + VB, :] + sc[p] * dm

    def sib_copy(c, t):
        return pltpu.make_async_remote_copy(
            src_ref=part.at[c, t, 1 - core], dst_ref=got_sib.at[c, t], send_sem=sib_send.at[c, t], recv_sem=sib_recv.at[c, t],
            device_id={'ens': sib}, device_id_type=MESH)

    def chip_copy(c, t):
        return pltpu.make_async_remote_copy(
            src_ref=chip.at[c, t], dst_ref=got_chip.at[c, t], send_sem=chip_send.at[c, t], recv_sem=chip_recv.at[c, t],
            device_id={'ens': mate}, device_id_type=MESH)

    def tot_copy(c, t):
        return pltpu.make_async_remote_copy(
            src_ref=tot.at[c, t, core], dst_ref=tot.at[c, t, core], send_sem=tot_send.at[c, t], recv_sem=tot_recv.at[c, t],
            device_id={'ens': sib}, device_id_type=MESH)

    def out_copy(t):
        rows = pl.ds(pl.multiple_of(t * CHUNK, CHUNK), CHUNK)
        return pltpu.make_async_copy(h.at[:, rows, :], out_hbm.at[:, rows, :], out_sem.at[t])

    def first_merge(c, t):
        sib_copy(c, t).wait_recv()
        merge(chip.at[c, t], part.at[c, t, core], got_sib.at[c, t], loc_members / 2)
        chip_copy(c, t).start()

    def second_merge(c, t):
        chip_copy(c, t).wait_recv()
        merge(tot.at[c, t, core], chip.at[c, t], got_chip.at[c, t], loc_members)
        tot_copy(c, t).start()

    def update(c, t):
        off = pl.multiple_of(t * CHUNK, CHUNK)
        tot_copy(c, t).wait_recv()

        def pair(r):
            return jnp.concatenate([tot[c, t, b, r:r + 1, :] for b in range(2)], axis=0)

        def obs_pair(ref, p):
            return jnp.concatenate([ref[p:p + 1, b * BLK:(b + 1) * BLK] for b in range(2)], axis=0)

        cov = {pq: pair(ROWS_C + n) for n, pq in enumerate(PAIRS)}
        rinv = [obs_pair(rinv_all.at[t], p) for p in range(OBS)]
        innov = [obs_pair(obs_all.at[t, c], p) - pair(ROWS_O + p) for p in range(OBS)]
        a, g, e = ns_weights(cov, rinv, innov, infl_ref[0], members)
        coef[0] = a
        for p in range(OBS):
            coef[1 + p] = e[p]
        for n, pq in enumerate(PAIRS):
            coef[1 + OBS + n] = g[pq]
        for b in range(2):
            rows = pl.ds(pl.multiple_of(off + b * BLK, BLK), BLK)
            for k in range(loc_members):
                for p in range(OBS):
                    yrow[b, k * OBS + p] = ht[t, b, pl.ds(k * nv + obs_i[p], 1), :] - tot[c, t, b, ROWS_O + p:ROWS_O + p + 1, :]
            ca = coef[0, b:b + 1, :]
            ce = [coef[1 + p, b:b + 1, :] for p in range(OBS)]
            cg = {pq: coef[1 + OBS + n, b:b + 1, :] for n, pq in enumerate(PAIRS)}
            for v in range(0, nv, VB):
                m = tot[c, t, b, v:v + VB, :]
                mom = [tot[c, t, b, (p + 1) * BLK + v:(p + 1) * BLK + v + VB, :] for p in range(OBS)]
                base = m + sum(ce[p] * mom[p] for p in range(OBS))
                mix = [sum(cg[sym(p, q)] * mom[q] for q in range(OBS)) for p in range(OBS)]
                for k in range(loc_members):
                    r = k * nv + v
                    new = base + ca * (ht[t, b, r:r + VB, :] - m)
                    for p in range(OBS):
                        new = new + yrow[b, k * OBS + p] * mix[p]
                    ht[t, b, r:r + VB, :] = new
            for k in range(loc_members):
                blk = ht[t, b, k * nv:(k + 1) * nv, :].T
                h[k, rows, :] = blk
                hb[0, rows, k * nv:(k + 1) * nv] = blk.astype(BF16)

    def cycle(c, _):
        for l in range(n_layers - 1):
            def full(t, _, l=l):
                layer_rows(l, t, WIDE, l % 2, False)
                return 0
            lax.fori_loop(0, cols // WIDE, full, 0)

        def last(t, _):
            layer_rows(n_layers - 1, t, CHUNK, (n_layers - 1) % 2, True)
            stats(c, t)
            sib_copy(c, t).start()

            @pl.when(t > 0)
            def _():
                first_merge(c, t - 1)
            return 0
        lax.fori_loop(0, n_chunks, last, 0)
        first_merge(c, n_chunks - 1)

        @pl.when(c == 0)
        def _():
            for step in range(1, n_dev):
                for copy in obs_copies(step):
                    copy.wait()

        def finish(t, _):
            second_merge(c, t)
            update(c, t)

            @pl.when(c == n_cycles - 1)
            def _():
                out_copy(t).start()
            return 0
        lax.fori_loop(0, n_chunks, finish, 0)

        def drain(t, _):
            sib_copy(c, t).wait_send()
            chip_copy(c, t).wait_send()
            tot_copy(c, t).wait_send()
            return 0
        lax.fori_loop(0, n_chunks, drain, 0)
        return 0
    lax.fori_loop(0, n_cycles, cycle, 0)
    for t in range(n_chunks):
        out_copy(t).wait()


def solution(mesh):
    n_dev = mesh.shape['ens']

    def per_device(x_loc, col_mix, w_in, w_out, obs_loc, rinv_loc, obs_idx, inflation):
        loc, cols, nv = x_loc.shape
        layers, _, ff = w_in.shape
        cycles = obs_loc.shape[0]
        n_chunks = cols // CHUNK
        rinv_t = rinv_loc.T
        obs_t = jnp.swapaxes(obs_loc, 1, 2)
        vm = pl.BlockSpec(memory_space=pltpu.VMEM)
        sm = pl.BlockSpec(memory_space=pltpu.SMEM)
        hbm = pl.BlockSpec(memory_space=pl.ANY)
        dma = pltpu.SemaphoreType.DMA
        packet = (PACK, BLK)
        f32 = jnp.float32
        return pl.pallas_call(
            functools.partial(kernel, n_dev, cycles, loc * n_dev),
            out_shape=jax.ShapeDtypeStruct(x_loc.shape, x_loc.dtype),
            in_specs=[pl.BlockSpec(memory_space=pltpu.HBM)] * 4 + [vm] * 2 + [sm] * 2,
            out_specs=hbm,
            scratch_shapes=[
                pltpu.VMEM((cols, cols), BF16),
                pltpu.VMEM((layers, nv, ff), BF16),
                pltpu.VMEM((layers, ff, nv), BF16),
                pltpu.VMEM((loc, cols, nv), f32),
                pltpu.VMEM((2, cols, loc * nv), BF16),
                pltpu.VMEM((n_chunks, 2, loc * nv, BLK), f32),
                pltpu.VMEM((WIDE, loc * nv), BF16),
                pltpu.VMEM((2, WIDE, ff), BF16),
                pltpu.VMEM((n_dev,) + rinv_t.shape, f32),
                pltpu.VMEM((n_dev,) + obs_t.shape, f32),
                pltpu.VMEM((cycles, n_chunks, 2) + packet, f32),
                pltpu.VMEM((cycles, n_chunks) + packet, f32),
                pltpu.VMEM((cycles, n_chunks) + packet, f32),
                pltpu.VMEM((cycles, n_chunks) + packet, f32),
                pltpu.VMEM((cycles, n_chunks, 2) + packet, f32),
                pltpu.VMEM((16, 2, BLK), f32),
                pltpu.VMEM((2, loc * OBS, 1, BLK), f32),
                dma((4,)), dma((n_chunks,)),
                dma((n_dev - 1, 2)), dma((n_dev - 1, 2)),
                dma((cycles, n_chunks)), dma((cycles, n_chunks)),
                dma((cycles, n_chunks)), dma((cycles, n_chunks)),
                dma((cycles, n_chunks)), dma((cycles, n_chunks)),
            ],
            compiler_params=pltpu.CompilerParams(collective_id=0, has_side_effects=True, vmem_limit_bytes=62 * 1024 * 1024),
        )(x_loc, col_mix, w_in, w_out, rinv_t, obs_t, obs_idx, inflation)

    state_spec = P(('case', 'ens'), None, None)
    in_specs = (state_spec, P(), P(), P(), P(None, ('case', 'ens'), None), P(('case', 'ens'), None), P(), P())
    return jax.shard_map(per_device, mesh=mesh, in_specs=in_specs, out_specs=state_spec, check_vma=False)
```

```python
import functools
import math
import jax
import jax.numpy as jnp
from jax import lax
from jax.experimental import pallas as pl
from jax.experimental.pallas import tpu as pltpu
from jax.sharding import PartitionSpec as P

NS_STEPS = 12
OBS = 4
PAIRS = [(p, q) for p in range(OBS) for q in range(p, OBS)]


def sym(p, q):
    return (p, q) if p <= q else (q, p)


def smul(a, b):
    return {(p, q): sum(a[sym(p, t)] * b[sym(t, q)] for t in range(OBS)) for p, q in PAIRS}


def shift(c, a):
    return {pq: (v + c if pq[0] == pq[1] else v) for pq, v in a.items()}


def scale_add(x, a, y, b):
    return {pq: x * a[pq] + y * b[pq] for pq in a}


def ns_weights(cov, rinv, innov, inflation, members):
    root_r = [jnp.sqrt(r) for r in rinv]
    c_mat = {(p, q): cov[(p, q)] * root_r[p] * root_r[q] for p, q in PAIRS}
    base = (members - 1) / inflation
    hat = shift(base, c_mat)
    norm2 = (members - OBS) * base * base
    for (p, q), v in hat.items():
        norm2 = norm2 + (v * v if p == q else 2.0 * (v * v))
    norm = jnp.sqrt(norm2)
    inv = 1.0 / norm
    rho, r_low, r_hat = base * inv, None, {pq: v * inv for pq, v in hat.items()}
    zero = jnp.zeros_like(inv)
    r_low = {pq: (inv if pq[0] == pq[1] else zero) for pq in PAIRS}
    zeta, z_low = jnp.ones_like(inv), {pq: zero for pq in PAIRS}
    for _ in range(NS_STEPS):
        prod = smul(z_low, r_hat)
        t_low = {pq: -0.5 * (zeta * r_low[pq] + prod[pq]) for pq in PAIRS}
        tau = 1.5 - 0.5 * (zeta * rho)
        t_hat = shift(tau, smul(c_mat, t_low))
        pr, pz = smul(r_low, t_hat), smul(z_low, t_hat)
        r_low = {pq: rho * t_low[pq] + pr[pq] for pq in PAIRS}
        z_low = {pq: zeta * t_low[pq] + pz[pq] for pq in PAIRS}
        rho, zeta = rho * tau, zeta * tau
        r_hat = shift(rho, smul(c_mat, r_low))
    inv_root = 1.0 / jnp.sqrt(norm)
    zs = zeta * inv_root
    q_mat = {pq: v * inv_root for pq, v in z_low.items()}
    s_hat = shift(zs, smul(c_mat, q_mat))
    vec = [root_r[p] * innov[p] for p in range(OBS)]
    for _ in range(2):
        vec = [sum(s_hat[sym(p, q)] * vec[q] for q in range(OBS)) for p in range(OBS)]
    fac = math.sqrt(members - 1)
    a = fac * zs
    g = {(p, q): fac * root_r[p] * root_r[q] * q_mat[(p, q)] for p, q in PAIRS}
    e = [root_r[p] * vec[p] for p in range(OBS)]
    return a, g, e


MESH = pl.DeviceIdType.MESH
CHUNK = 256
BLK = 128
ROWS_O = 5 * BLK
ROWS_C = ROWS_O + OBS
PACK = ROWS_O + 16
VB = 16
BF16 = jnp.bfloat16


def dot(a, b):
    return jnp.dot(a, b, preferred_element_type=jnp.float32)


def gelu_of_half(z):
    return z + z * jnp.tanh(z * (2 * 0.7978845608028654 + (8 * 0.035677408136300125) * (z * z)))


def kernel(n_dev, n_cycles, members, x_hbm, a_hbm, w_hbm, u_hbm, rinv_ref, obs_ref, idx_ref, infl_ref, h,
           av, wv, uv, hb, ht, mb, hid, macc, rinv_all, obs_all, part, got_sib, chip, got_chip, tot, yrow,
           load_sem, obs_send, obs_recv, sib_send, sib_recv, chip_send, chip_recv, tot_send, tot_recv):
    loc_members, cols, nv = h.shape
    n_layers = wv.shape[0]
    n_chunks = cols // CHUNK
    me = lax.axis_index('ens')
    core = lax.rem(me, 2)
    sib = me + 1 - 2 * core
    mate = lax.rem(me + 2, n_dev)
    obs_i = [idx_ref[p] for p in range(OBS)]

    loads = [pltpu.make_async_copy(src, dst, load_sem.at[i]) for i, (src, dst) in enumerate(((x_hbm, h), (a_hbm, av), (w_hbm, wv), (u_hbm, uv)))]
    for load in loads:
        load.start()

    barrier = pltpu.get_barrier_semaphore()
    for step in range(1, n_dev):
        pl.semaphore_signal(barrier, inc=1, device_id={'ens': lax.rem(me + step, n_dev)}, device_id_type=MESH)

    def obs_copies(step):
        dev = {'ens': lax.rem(me + step, n_dev)}
        return [pltpu.make_async_remote_copy(src_ref=src, dst_ref=dst.at[me], send_sem=obs_send.at[step - 1, i], recv_sem=obs_recv.at[step - 1, i],
                                             device_id=dev, device_id_type=MESH)
                for i, (src, dst) in enumerate(((rinv_ref, rinv_all), (obs_ref, obs_all)))]

    loads[0].wait()
    for k in range(loc_members):
        hb[0, :, k * nv:(k + 1) * nv] = h[k].astype(BF16)
    loads[2].wait()
    wv[...] = wv[...] * jnp.bfloat16(0.5)
    loads[3].wait()
    loads[1].wait()

    def mixed(off, rows, src):
        return dot(av[pl.ds(off, rows), :], hb[src]).astype(BF16)

    def layer_rows(l, off, rows, src, put):
        for s in range(loc_members + 1):
            if s < loc_members:
                pre = dot(mb[0:rows, s * nv:(s + 1) * nv], wv[l])
            if s >= 1:
                k = s - 1
                put(k, h[k, pl.ds(off, rows), :] + dot(hid[k % 2, 0:rows, :], uv[l]))
            if s < loc_members:
                hid[s % 2, 0:rows, :] = gelu_of_half(pre).astype(BF16)

    def full_layer(l, c):
        src = l % 2
        mb[...] = mixed(0, cols, src) if l > 0 or c == 0 else macc[...].astype(BF16)

        def put(k, new):
            h[k] = new
            hb[1 - src, :, k * nv:(k + 1) * nv] = new.astype(BF16)
        layer_rows(l, 0, cols, src, put)

    def last_layer(t, b):
        l = n_layers - 1
        off = pl.multiple_of(t * CHUNK + b * BLK, BLK)
        mb[0:BLK, :] = mixed(off, BLK, l % 2)

        def put(k, new):
            ht[t, b, k * nv:(k + 1) * nv, :] = new.T
        layer_rows(l, off, BLK, l % 2, put)

    def stats(c, t, b):
        ho = [[ht[t, b, pl.ds(k * nv + obs_i[p], 1), :] for k in range(loc_members)] for p in range(OBS)]
        mo = [sum(x[1:], x[0]) * (1.0 / loc_members) for x in ho]
        y = [[x - mo[p] for x in ho[p]] for p in range(OBS)]
        for p in range(OBS):
            part[c, t, b, ROWS_O + p:ROWS_O + p + 1, :] = mo[p]
        for n, (p, q) in enumerate(PAIRS):
            part[c, t, b, ROWS_C + n:ROWS_C + n + 1, :] = sum(y[p][k] * y[q][k] for k in range(loc_members))
        for v in range(0, nv, VB):
            x = [ht[t, b, k * nv + v:k * nv + v + VB, :] for k in range(loc_members)]
            m = sum(x[1:], x[0]) * (1.0 / loc_members)
            d = [z - m for z in x]
            part[c, t, b, v:v + VB, :] = m
            for p in range(OBS):
                o = (p + 1) * BLK + v
                part[c, t, b, o:o + VB, :] = sum(y[p][k] * d[k] for k in range(loc_members))

    def merge(dst, one, two, half_n):
        da = [two[ROWS_O + p:ROWS_O + p + 1, :] - one[ROWS_O + p:ROWS_O + p + 1, :] for p in range(OBS)]
        for p in range(OBS):
            r = ROWS_O + p
            dst[r:r + 1, :] = 0.5 * (one[r:r + 1, :] + two[r:r + 1, :])
        for n, (p, q) in enumerate(PAIRS):
            r = ROWS_C + n
            dst[r:r + 1, :] = one[r:r + 1, :] + two[r:r + 1, :] + (half_n * da[p]) * da[q]
        sc = [half_n * x for x in da]
        for v in range(0, nv, VB):
            ma, mbb = one[v:v + VB, :], two[v:v + VB, :]
            dst[v:v + VB, :] = 0.5 * (ma + mbb)
            dm = mbb - ma
            for p in range(OBS):
                o = (p + 1) * BLK + v
                dst[o:o + VB, :] = one[o:o + VB, :] + two[o:o + VB, :] + sc[p] * dm

    def sib_copy(c, t):
        return pltpu.make_async_remote_copy(
            src_ref=part.at[c, t, 1 - core], dst_ref=got_sib.at[c, t], send_sem=sib_send.at[c, t], recv_sem=sib_recv.at[c, t],
            device_id={'ens': sib}, device_id_type=MESH)

    def chip_copy(c, t):
        return pltpu.make_async_remote_copy(
            src_ref=chip.at[c, t], dst_ref=got_chip.at[c, t], send_sem=chip_send.at[c, t], recv_sem=chip_recv.at[c, t],
            device_id={'ens': mate}, device_id_type=MESH)

    def tot_copy(c, t):
        return pltpu.make_async_remote_copy(
            src_ref=tot.at[c, t, core], dst_ref=tot.at[c, t, core], send_sem=tot_send.at[c, t], recv_sem=tot_recv.at[c, t],
            device_id={'ens': sib}, device_id_type=MESH)

    def first_merge(c, t):
        sib_copy(c, t).wait_recv()
        merge(chip.at[c, t], part.at[c, t, core], got_sib.at[c, t], loc_members / 2)
        chip_copy(c, t).start()

    def second_merge(c, t):
        chip_copy(c, t).wait_recv()
        merge(tot.at[c, t, core], chip.at[c, t], got_chip.at[c, t], loc_members)
        tot_copy(c, t).start()

    def update(c, t, b):
        lanes = pl.ds(pl.multiple_of(b * BLK, BLK), BLK)
        rows = pl.ds(pl.multiple_of(t * CHUNK + b * BLK, BLK), BLK)

        def row(r):
            return tot[c, t, b, r:r + 1, :]

        cov = {pq: row(ROWS_C + n) for n, pq in enumerate(PAIRS)}
        rinv = [rinv_all[t, p:p + 1, lanes] for p in range(OBS)]
        innov = [obs_all[t, c, p:p + 1, lanes] - row(ROWS_O + p) for p in range(OBS)]
        ca, cg, ce = ns_weights(cov, rinv, innov, infl_ref[0], members)
        for k in range(loc_members):
            for p in range(OBS):
                yrow[k * OBS + p] = ht[t, b, pl.ds(k * nv + obs_i[p], 1), :] - row(ROWS_O + p)
        for v in range(0, nv, VB):
            m = tot[c, t, b, v:v + VB, :]
            mom = [tot[c, t, b, (p + 1) * BLK + v:(p + 1) * BLK + v + VB, :] for p in range(OBS)]
            base = m + sum(ce[p] * mom[p] for p in range(OBS))
            mix = [sum(cg[sym(p, q)] * mom[q] for q in range(OBS)) for p in range(OBS)]
            for k in range(loc_members):
                r = k * nv + v
                new = base + ca * (ht[t, b, r:r + VB, :] - m)
                for p in range(OBS):
                    new = new + yrow[k * OBS + p] * mix[p]
                ht[t, b, r:r + VB, :] = new
        for k in range(loc_members):
            blk = ht[t, b, k * nv:(k + 1) * nv, :].T
            h[k, rows, :] = blk
            if c < n_cycles - 1:
                hb[0, rows, k * nv:(k + 1) * nv] = blk.astype(BF16)

    for c in range(n_cycles):
        for l in range(n_layers - 1):
            full_layer(l, c)
            if c == 0 and l == 0:
                pl.semaphore_wait(barrier, n_dev - 1)
                for step in range(1, n_dev):
                    for copy in obs_copies(step):
                        copy.start()
                rinv_all[me] = rinv_ref[...]
                obs_all[me] = obs_ref[...]

        def last(t, _, c=c):
            last_layer(t, 1 - core)
            stats(c, t, 1 - core)
            sib_copy(c, t).start()
            last_layer(t, core)
            stats(c, t, core)
            first_merge(c, t)
            return 0
        lax.fori_loop(0, n_chunks, last, 0)

        if c == 0:
            for step in range(1, n_dev):
                for copy in obs_copies(step):
                    copy.wait()
        if c < n_cycles - 1:
            macc[...] = jnp.zeros_like(macc)

        def finish(t, _, c=c):
            second_merge(c, t)
            update(c, t, core)
            tot_copy(c, t).wait_recv()
            update(c, t, 1 - core)
            if c < n_cycles - 1:
                span = pl.ds(pl.multiple_of(t * CHUNK, CHUNK), CHUNK)
                for r in range(0, cols, CHUNK):
                    macc[r:r + CHUNK, :] += dot(av[r:r + CHUNK, span], hb[0, span, :])
            return 0
        lax.fori_loop(0, n_chunks, finish, 0)

        def drain(t, _, c=c):
            sib_copy(c, t).wait_send()
            chip_copy(c, t).wait_send()
            tot_copy(c, t).wait_send()
            return 0
        lax.fori_loop(0, n_chunks, drain, 0)


def solution(mesh):
    n_dev = mesh.shape['ens']

    def per_device(x_loc, col_mix, w_in, w_out, obs_loc, rinv_loc, obs_idx, inflation):
        loc, cols, nv = x_loc.shape
        layers, _, ff = w_in.shape
        cycles = obs_loc.shape[0]
        n_chunks = cols // CHUNK
        rinv_t = rinv_loc.T
        obs_t = jnp.swapaxes(obs_loc, 1, 2)
        vm = pl.BlockSpec(memory_space=pltpu.VMEM)
        sm = pl.BlockSpec(memory_space=pltpu.SMEM)
        dma = pltpu.SemaphoreType.DMA
        packet = (PACK, BLK)
        f32 = jnp.float32
        return pl.pallas_call(
            functools.partial(kernel, n_dev, cycles, loc * n_dev),
            out_shape=pltpu.VMEM(x_loc.shape, x_loc.dtype),
            in_specs=[pl.BlockSpec(memory_space=pltpu.HBM)] * 4 + [vm] * 2 + [sm] * 2,
            out_specs=vm,
            scratch_shapes=[
                pltpu.VMEM((cols, cols), BF16),
                pltpu.VMEM((layers, nv, ff), BF16),
                pltpu.VMEM((layers, ff, nv), BF16),
                pltpu.VMEM((2, cols, loc * nv), BF16),
                pltpu.VMEM((n_chunks, 2, loc * nv, BLK), f32),
                pltpu.VMEM((cols, loc * nv), BF16),
                pltpu.VMEM((2, cols, ff), BF16),
                pltpu.VMEM((cols, loc * nv), f32),
                pltpu.VMEM((n_dev,) + rinv_t.shape, f32),
                pltpu.VMEM((n_dev,) + obs_t.shape, f32),
                pltpu.VMEM((cycles, n_chunks, 2) + packet, f32),
                pltpu.VMEM((cycles, n_chunks) + packet, f32),
                pltpu.VMEM((cycles, n_chunks) + packet, f32),
                pltpu.VMEM((cycles, n_chunks) + packet, f32),
                pltpu.VMEM((cycles, n_chunks, 2) + packet, f32),
                pltpu.VMEM((loc * OBS, 1, BLK), f32),
                dma((4,)),
                dma((n_dev - 1, 2)), dma((n_dev - 1, 2)),
                dma((cycles, n_chunks)), dma((cycles, n_chunks)),
                dma((cycles, n_chunks)), dma((cycles, n_chunks)),
                dma((cycles, n_chunks)), dma((cycles, n_chunks)),
            ],
            compiler_params=pltpu.CompilerParams(collective_id=0, has_side_effects=True, vmem_limit_bytes=58 * 1024 * 1024),
        )(x_loc, col_mix, w_in, w_out, rinv_t, obs_t, obs_idx, inflation)

    state_spec = P(('case', 'ens'), None, None)
    in_specs = (state_spec, P(), P(), P(), P(None, ('case', 'ens'), None), P(('case', 'ens'), None), P(), P())
    return jax.shard_map(per_device, mesh=mesh, in_specs=in_specs, out_specs=state_spec, check_vma=False)
```

```python
import functools
import math
import jax
import jax.numpy as jnp
from jax import lax
from jax.experimental import pallas as pl
from jax.experimental.pallas import tpu as pltpu
from jax.sharding import PartitionSpec as P

NS_STEPS = 12
OBS = 4
PAIRS = [(p, q) for p in range(OBS) for q in range(p, OBS)]


def sym(p, q):
    return (p, q) if p <= q else (q, p)


def smul(a, b):
    return {(p, q): sum(a[sym(p, t)] * b[sym(t, q)] for t in range(OBS)) for p, q in PAIRS}


def shift(c, a):
    return {pq: (v + c if pq[0] == pq[1] else v) for pq, v in a.items()}


def ns_weights(cov, rinv, innov, inflation, members):
    root_r = [jnp.sqrt(r) for r in rinv]
    base = (members - 1) / inflation
    b_hat = shift(base, {(p, q): cov[(p, q)] * root_r[p] * root_r[q] for p, q in PAIRS})
    norm2 = (members - OBS) * base * base
    for (p, q), v in b_hat.items():
        norm2 = norm2 + (v * v if p == q else 2.0 * (v * v))
    norm = jnp.sqrt(norm2)
    inv = 1.0 / norm
    full = (8, inv.shape[1])
    sub = lax.broadcasted_iota(jnp.int32, full, 0)

    def spread(x):
        return jnp.broadcast_to(x, full)

    state = {}
    for p, q in PAIRS:
        rest = jnp.where(sub == 1, spread(inv), jnp.where(sub == 2, 1.0, 0.0)) if p == q else jnp.zeros(full, jnp.float32)
        state[(p, q)] = jnp.where(sub == 0, spread(b_hat[(p, q)] * inv), rest)
    coef = jnp.where(sub == 1, spread(base * inv), jnp.where(sub == 3, 1.0, 0.0))
    for step in range(NS_STEPS):
        tau = 1.5 - 0.5 * spread(coef[1:2])
        t_hat = shift(1.5, {pq: -0.5 * spread(v[0:1]) for pq, v in state.items()})
        t_low = {pq: -0.5 * spread(v[1:2]) for pq, v in state.items()}
        prod = smul(state, t_hat)
        state = {pq: prod[pq] + coef * t_low[pq] for pq in PAIRS}
        coef = coef * tau
        if step < NS_STEPS - 1:
            prod = smul(state, t_hat)
            state = {pq: jnp.where(sub < 2, prod[pq] + coef * t_low[pq], state[pq]) for pq in PAIRS}
            coef = jnp.where(sub < 2, coef * tau, coef)
    inv_root = 1.0 / jnp.sqrt(norm)
    s_hat = {pq: v[2:3] * inv_root for pq, v in state.items()}
    q_mat = {pq: v[3:4] * inv_root for pq, v in state.items()}
    vec = [root_r[p] * innov[p] for p in range(OBS)]
    for _ in range(2):
        vec = [sum(s_hat[sym(p, q)] * vec[q] for q in range(OBS)) for p in range(OBS)]
    fac = math.sqrt(members - 1)
    a = fac * (coef[3:4] * inv_root)
    g = {(p, q): fac * root_r[p] * root_r[q] * q_mat[(p, q)] for p, q in PAIRS}
    e = [root_r[p] * vec[p] for p in range(OBS)]
    return a, g, e


MESH = pl.DeviceIdType.MESH
CHUNK = 256
BLK = 128
ROWS_O = 5 * BLK
ROWS_C = ROWS_O + OBS
PART = ROWS_O + 8
TOTAL = ROWS_O + 16
VB = 16
BF16 = jnp.bfloat16


def dot(a, b):
    return jnp.dot(a, b, preferred_element_type=jnp.float32)


def gelu_of_half(z):
    return z + z * jnp.tanh(z * (2 * 0.7978845608028654 + (8 * 0.035677408136300125) * (z * z)))


def kernel(n_dev, n_cycles, members, x_hbm, a_hbm, w_hbm, u_hbm, rinv_hbm, obs_hbm, idx_ref, infl_ref, h,
           av, wv, uv, hb, ht, mb, hid, macc, rinv_all, obs_all, part, got_sib, chip, got_chip, tot, mrow, arow, yrow,
           load_sem, obs_send, obs_recv, sib_send, sib_recv, chip_send, chip_recv, tot_send, tot_recv):
    loc_members, cols, nv = h.shape
    n_layers = wv.shape[0]
    n_chunks = cols // CHUNK
    me = lax.axis_index('ens')
    core = lax.rem(me, 2)
    sib = me + 1 - 2 * core
    mate = lax.rem(me + 2, n_dev)
    obs_i = [idx_ref[p] for p in range(OBS)]

    pairs = [(a_hbm, av)] + [(x_hbm.at[k], h.at[k]) for k in range(loc_members)] + [
        (w_hbm, wv), (u_hbm, uv), (rinv_hbm, rinv_all.at[me]), (obs_hbm, obs_all.at[me])]
    loads = [pltpu.make_async_copy(src, dst, load_sem.at[i]) for i, (src, dst) in enumerate(pairs)]
    load_a, load_x, load_w, load_u, load_obs = loads[0], loads[1:1 + loc_members], loads[-4], loads[-3], loads[-2:]
    for load in loads:
        load.start()

    barrier = pltpu.get_barrier_semaphore()
    for step in range(1, n_dev):
        pl.semaphore_signal(barrier, inc=1, device_id={'ens': lax.rem(me + step, n_dev)}, device_id_type=MESH)

    def obs_copies(step):
        dev = {'ens': lax.rem(me + step, n_dev)}
        return [pltpu.make_async_remote_copy(src_ref=ref.at[me], dst_ref=ref.at[me], send_sem=obs_send.at[step - 1, i],
                                             recv_sem=obs_recv.at[step - 1, i], device_id=dev, device_id_type=MESH)
                for i, ref in enumerate((rinv_all, obs_all))]

    def mixed(off, rows, src):
        return dot(av[pl.ds(off, rows), :], hb[src]).astype(BF16)

    def layer_rows(l, off, rows, src, put):
        for s in range(loc_members + 1):
            if s < loc_members:
                pre = dot(mb[0:rows, s * nv:(s + 1) * nv], wv[l])
            if s >= 1:
                k = s - 1
                put(k, h[k, pl.ds(off, rows), :] + dot(hid[k % 2, 0:rows, :], uv[l]))
            if s < loc_members:
                hid[s % 2, 0:rows, :] = gelu_of_half(pre).astype(BF16)

    def full_layer(l, c):
        src = l % 2
        if c == 0 and l == 0:
            load_a.wait()
            for i in range(loc_members):
                load_x[i].wait()
                hb[0, :, i * nv:(i + 1) * nv] = h[i].astype(BF16)
            mb[...] = mixed(0, cols, src)
            load_w.wait()
            wv[...] = wv[...] * jnp.bfloat16(0.5)
            load_u.wait()
        elif l == 0:
            mb[...] = macc[...].astype(BF16)
        else:
            mb[...] = mixed(0, cols, src)

        def put(k, new):
            h[k] = new
            hb[1 - src, :, k * nv:(k + 1) * nv] = new.astype(BF16)
        layer_rows(l, 0, cols, src, put)

    def last_layer(t, b):
        l = n_layers - 1
        off = pl.multiple_of(t * CHUNK + b * BLK, BLK)
        mb[0:BLK, :] = mixed(off, BLK, l % 2)

        def put(k, new):
            ht[t, b, k * nv:(k + 1) * nv, :] = new.T
        layer_rows(l, off, BLK, l % 2, put)

    def stats(c, t, b):
        ho = [[ht[t, b, pl.ds(k * nv + obs_i[p], 1), :] for k in range(loc_members)] for p in range(OBS)]
        mo = [sum(x[1:], x[0]) * (1.0 / loc_members) for x in ho]
        y = [[x - mo[p] for x in ho[p]] for p in range(OBS)]
        for p in range(OBS):
            part[c, t, b, ROWS_O + p:ROWS_O + p + 1, :] = mo[p]
        for v in range(0, nv, VB):
            x = [ht[t, b, k * nv + v:k * nv + v + VB, :] for k in range(loc_members)]
            m = sum(x[1:], x[0]) * (1.0 / loc_members)
            d = [z - m for z in x]
            part[c, t, b, v:v + VB, :] = m
            for p in range(OBS):
                o = (p + 1) * BLK + v
                part[c, t, b, o:o + VB, :] = sum(y[p][k] * d[k] for k in range(loc_members))

    def merge(dst, one, two, two_o, half_n, keep):
        for p in range(OBS):
            r = ROWS_O + p
            dst[r:r + 1, :] = 0.5 * (one[r:r + 1, :] + two_o[p])
        sc = [half_n * (two_o[p] - one[ROWS_O + p:ROWS_O + p + 1, :]) for p in range(OBS)]
        for v in range(0, nv, VB):
            ma, mbb = one[v:v + VB, :], two[v:v + VB, :]
            dst[v:v + VB, :] = 0.5 * (ma + mbb)
            dm = mbb - ma
            for p in range(OBS):
                o = (p + 1) * BLK + v
                val = one[o:o + VB, :] + two[o:o + VB, :] + sc[p] * dm
                dst[o:o + VB, :] = val
                if keep:
                    arow[o - BLK:o - BLK + VB, :] = val
        if keep:
            for n, (p, q) in enumerate(PAIRS):
                dst[ROWS_C + n:ROWS_C + n + 1, :] = arow[pl.ds(p * BLK + obs_i[q], 1), :]

    def sib_copy(c, t):
        return pltpu.make_async_remote_copy(
            src_ref=part.at[c, t, 1 - core], dst_ref=got_sib.at[c, t], send_sem=sib_send.at[c, t], recv_sem=sib_recv.at[c, t],
            device_id={'ens': sib}, device_id_type=MESH)

    def chip_copy(c, t):
        return pltpu.make_async_remote_copy(
            src_ref=chip.at[c, t, 0:ROWS_O], dst_ref=got_chip.at[c, t], send_sem=chip_send.at[c, t], recv_sem=chip_recv.at[c, t],
            device_id={'ens': mate}, device_id_type=MESH)

    def tot_copy(c, t):
        return pltpu.make_async_remote_copy(
            src_ref=tot.at[c, t, core], dst_ref=tot.at[c, t, core], send_sem=tot_send.at[c, t], recv_sem=tot_recv.at[c, t],
            device_id={'ens': sib}, device_id_type=MESH)

    def first_merge(c, t):
        sib_copy(c, t).wait_recv()
        two = got_sib.at[c, t]
        two_o = [two[ROWS_O + p:ROWS_O + p + 1, :] for p in range(OBS)]
        merge(chip.at[c, t], part.at[c, t, core], two, two_o, loc_members / 2, False)
        chip_copy(c, t).start()

    def second_merge(c, t):
        chip_copy(c, t).wait_recv()
        two = got_chip.at[c, t]
        mrow[...] = two[0:BLK, :]
        two_o = [mrow[pl.ds(obs_i[p], 1), :] for p in range(OBS)]
        merge(tot.at[c, t, core], chip.at[c, t], two, two_o, loc_members, True)
        tot_copy(c, t).start()

    def update(c, t, b):
        lanes = pl.ds(pl.multiple_of(b * BLK, BLK), BLK)
        rows = pl.ds(pl.multiple_of(t * CHUNK + b * BLK, BLK), BLK)

        def row(r):
            return tot[c, t, b, r:r + 1, :]

        cov = {pq: row(ROWS_C + n) for n, pq in enumerate(PAIRS)}
        rinv = [rinv_all[t, p:p + 1, lanes] for p in range(OBS)]
        innov = [obs_all[t, c, p:p + 1, lanes] - row(ROWS_O + p) for p in range(OBS)]
        ca, cg, ce = ns_weights(cov, rinv, innov, infl_ref[0], members)
        for k in range(loc_members):
            for p in range(OBS):
                yrow[k * OBS + p] = ht[t, b, pl.ds(k * nv + obs_i[p], 1), :] - row(ROWS_O + p)
        for v in range(0, nv, VB):
            m = tot[c, t, b, v:v + VB, :]
            mom = [tot[c, t, b, (p + 1) * BLK + v:(p + 1) * BLK + v + VB, :] for p in range(OBS)]
            base = m + sum(ce[p] * mom[p] for p in range(OBS))
            mix = [sum(cg[sym(p, q)] * mom[q] for q in range(OBS)) for p in range(OBS)]
            for k in range(loc_members):
                r = k * nv + v
                new = base + ca * (ht[t, b, r:r + VB, :] - m)
                for p in range(OBS):
                    new = new + yrow[k * OBS + p] * mix[p]
                ht[t, b, r:r + VB, :] = new
        for k in range(loc_members):
            blk = ht[t, b, k * nv:(k + 1) * nv, :].T
            h[k, rows, :] = blk
            if c < n_cycles - 1:
                hb[0, rows, k * nv:(k + 1) * nv] = blk.astype(BF16)

    for c in range(n_cycles):
        for l in range(n_layers - 1):
            full_layer(l, c)
            if c == 0 and l == 0:
                for load in load_obs:
                    load.wait()
                pl.semaphore_wait(barrier, n_dev - 1)
                for step in range(1, n_dev):
                    for copy in obs_copies(step):
                        copy.start()

        def last(t, _, c=c):
            last_layer(t, 1 - core)
            stats(c, t, 1 - core)
            sib_copy(c, t).start()
            last_layer(t, core)
            stats(c, t, core)
            first_merge(c, t)
            return 0
        lax.fori_loop(0, n_chunks, last, 0)

        if c == 0:
            for step in range(1, n_dev):
                for copy in obs_copies(step):
                    copy.wait()
        if c < n_cycles - 1:
            macc[...] = jnp.zeros_like(macc)

        def finish(t, _, c=c):
            second_merge(c, t)
            update(c, t, core)
            tot_copy(c, t).wait_recv()
            update(c, t, 1 - core)
            if c < n_cycles - 1:
                span = pl.ds(pl.multiple_of(t * CHUNK, CHUNK), CHUNK)
                for r in range(0, cols, CHUNK):
                    macc[r:r + CHUNK, :] += dot(av[r:r + CHUNK, span], hb[0, span, :])
            return 0
        lax.fori_loop(0, n_chunks, finish, 0)

        def drain(t, _, c=c):
            sib_copy(c, t).wait_send()
            chip_copy(c, t).wait_send()
            tot_copy(c, t).wait_send()
            return 0
        lax.fori_loop(0, n_chunks, drain, 0)


def solution(mesh):
    n_dev = mesh.shape['ens']

    def per_device(x_loc, col_mix, w_in, w_out, obs_loc, rinv_loc, obs_idx, inflation):
        loc, cols, nv = x_loc.shape
        layers, _, ff = w_in.shape
        cycles = obs_loc.shape[0]
        n_chunks = cols // CHUNK
        rinv_t = rinv_loc.T
        obs_t = jnp.swapaxes(obs_loc, 1, 2)
        vm = pl.BlockSpec(memory_space=pltpu.VMEM)
        sm = pl.BlockSpec(memory_space=pltpu.SMEM)
        dma = pltpu.SemaphoreType.DMA
        f32 = jnp.float32
        return pl.pallas_call(
            functools.partial(kernel, n_dev, cycles, loc * n_dev),
            out_shape=pltpu.VMEM(x_loc.shape, x_loc.dtype),
            in_specs=[pl.BlockSpec(memory_space=pltpu.HBM)] * 6 + [sm] * 2,
            out_specs=vm,
            scratch_shapes=[
                pltpu.VMEM((cols, cols), BF16),
                pltpu.VMEM((layers, nv, ff), BF16),
                pltpu.VMEM((layers, ff, nv), BF16),
                pltpu.VMEM((2, cols, loc * nv), BF16),
                pltpu.VMEM((n_chunks, 2, loc * nv, BLK), f32),
                pltpu.VMEM((cols, loc * nv), BF16),
                pltpu.VMEM((2, cols, ff), BF16),
                pltpu.VMEM((cols, loc * nv), f32),
                pltpu.VMEM((n_dev,) + rinv_t.shape, f32),
                pltpu.VMEM((n_dev,) + obs_t.shape, f32),
                pltpu.VMEM((cycles, n_chunks, 2, PART, BLK), f32),
                pltpu.VMEM((cycles, n_chunks, PART, BLK), f32),
                pltpu.VMEM((cycles, n_chunks, PART, BLK), f32),
                pltpu.VMEM((cycles, n_chunks, ROWS_O, BLK), f32),
                pltpu.VMEM((cycles, n_chunks, 2, TOTAL, BLK), f32),
                pltpu.VMEM((BLK, BLK), f32),
                pltpu.VMEM((OBS * BLK, BLK), f32),
                pltpu.VMEM((loc * OBS, 1, BLK), f32),
                dma((loc + 5,)),
                dma((n_dev - 1, 2)), dma((n_dev - 1, 2)),
                dma((cycles, n_chunks)), dma((cycles, n_chunks)),
                dma((cycles, n_chunks)), dma((cycles, n_chunks)),
                dma((cycles, n_chunks)), dma((cycles, n_chunks)),
            ],
            compiler_params=pltpu.CompilerParams(collective_id=0, has_side_effects=True, vmem_limit_bytes=58 * 1024 * 1024),
        )(x_loc, col_mix, w_in, w_out, rinv_t, obs_t, obs_idx, inflation)

    state_spec = P(('case', 'ens'), None, None)
    in_specs = (state_spec, P(), P(), P(), P(None, ('case', 'ens'), None), P(('case', 'ens'), None), P(), P())
    return jax.shard_map(per_device, mesh=mesh, in_specs=in_specs, out_specs=state_spec, check_vma=False)
```

```python
import functools
import math
import jax
import jax.numpy as jnp
from jax import lax
from jax.experimental import pallas as pl
from jax.experimental.pallas import tpu as pltpu
from jax.sharding import PartitionSpec as P

NS_STEPS = 12
OBS = 4
PAIRS = [(p, q) for p in range(OBS) for q in range(p, OBS)]


def sym(p, q):
    return (p, q) if p <= q else (q, p)


def smul(a, b):
    return {(p, q): sum(a[sym(p, t)] * b[sym(t, q)] for t in range(OBS)) for p, q in PAIRS}


def shift(c, a):
    return {pq: (v + c if pq[0] == pq[1] else v) for pq, v in a.items()}


def ns_weights(cov, rinv, innov, inflation, members):
    root_r = [jnp.sqrt(r) for r in rinv]
    base = (members - 1) / inflation
    b_hat = shift(base, {(p, q): cov[(p, q)] * root_r[p] * root_r[q] for p, q in PAIRS})
    norm2 = (members - OBS) * base * base
    for (p, q), v in b_hat.items():
        norm2 = norm2 + (v * v if p == q else 2.0 * (v * v))
    norm = jnp.sqrt(norm2)
    inv = 1.0 / norm
    full = (8, inv.shape[1])
    sub = lax.broadcasted_iota(jnp.int32, full, 0)

    def spread(x):
        return jnp.broadcast_to(x, full)

    state = {}
    for p, q in PAIRS:
        rest = jnp.where(sub == 1, spread(inv), jnp.where(sub == 2, 1.0, 0.0)) if p == q else jnp.zeros(full, jnp.float32)
        state[(p, q)] = jnp.where(sub == 0, spread(b_hat[(p, q)] * inv), rest)
    coef = jnp.where(sub == 1, spread(base * inv), jnp.where(sub == 3, 1.0, 0.0))
    for step in range(NS_STEPS):
        tau = 1.5 - 0.5 * spread(coef[1:2])
        t_hat = shift(1.5, {pq: -0.5 * spread(v[0:1]) for pq, v in state.items()})
        t_low = {pq: -0.5 * spread(v[1:2]) for pq, v in state.items()}
        prod = smul(state, t_hat)
        state = {pq: prod[pq] + coef * t_low[pq] for pq in PAIRS}
        coef = coef * tau
        if step < NS_STEPS - 1:
            prod = smul(state, t_hat)
            state = {pq: jnp.where(sub < 2, prod[pq] + coef * t_low[pq], state[pq]) for pq in PAIRS}
            coef = jnp.where(sub < 2, coef * tau, coef)
    inv_root = 1.0 / jnp.sqrt(norm)
    s_hat = {pq: v[2:3] * inv_root for pq, v in state.items()}
    q_mat = {pq: v[3:4] * inv_root for pq, v in state.items()}
    vec = [root_r[p] * innov[p] for p in range(OBS)]
    for _ in range(2):
        vec = [sum(s_hat[sym(p, q)] * vec[q] for q in range(OBS)) for p in range(OBS)]
    fac = math.sqrt(members - 1)
    a = fac * (coef[3:4] * inv_root)
    g = {(p, q): fac * root_r[p] * root_r[q] * q_mat[(p, q)] for p, q in PAIRS}
    e = [root_r[p] * vec[p] for p in range(OBS)]
    return a, g, e


MESH = pl.DeviceIdType.MESH
CHUNK = 256
BLK = 128
ROWS_O = 5 * BLK
ROWS_C = ROWS_O + OBS
PART = ROWS_O + 8
TOTAL = ROWS_O + 16
VB = 16
BF16 = jnp.bfloat16


def dot(a, b):
    return jnp.dot(a, b, preferred_element_type=jnp.float32)


def gelu_of_half(z):
    return z + z * jnp.tanh(z * (2 * 0.7978845608028654 + (8 * 0.035677408136300125) * (z * z)))


def kernel(n_dev, n_cycles, members, x_hbm, a_hbm, w_hbm, u_hbm, rinv_hbm, obs_hbm, idx_ref, infl_ref, h,
           av, wv, uv, hb, ht, mb, hid, macc, rinv_all, obs_all, part, got_sib, chip, got_chip, tot, mrow, arow, yrow,
           load_sem, obs_send, obs_recv, sib_send, sib_recv, chip_send, chip_recv, tot_send, tot_recv):
    loc_members, cols, nv = h.shape
    n_layers = wv.shape[0]
    n_chunks = cols // CHUNK
    me = lax.axis_index('ens')
    core = lax.rem(me, 2)
    sib = me + 1 - 2 * core
    mate = lax.rem(me + 2, n_dev)
    obs_i = [idx_ref[p] for p in range(OBS)]

    def span(t):
        return pl.ds(pl.multiple_of(t * CHUNK, CHUNK), CHUNK)

    def load_x(t):
        return pltpu.make_async_copy(x_hbm.at[:, span(t), :], h.at[:, span(t), :], load_sem.at[t])

    loads = [pltpu.make_async_copy(src, dst, load_sem.at[n_chunks + i]) for i, (src, dst) in enumerate(
        ((a_hbm, av), (w_hbm, wv), (u_hbm, uv), (rinv_hbm, rinv_all.at[me]), (obs_hbm, obs_all.at[me])))]
    loads[0].start()
    load_x(0).start()
    load_x(1).start()

    barrier = pltpu.get_barrier_semaphore()
    for step in range(1, n_dev):
        pl.semaphore_signal(barrier, inc=1, device_id={'ens': lax.rem(me + step, n_dev)}, device_id_type=MESH)

    def obs_copies(step):
        dev = {'ens': lax.rem(me + step, n_dev)}
        return [pltpu.make_async_remote_copy(src_ref=ref.at[me], dst_ref=ref.at[me], send_sem=obs_send.at[step - 1, i],
                                             recv_sem=obs_recv.at[step - 1, i], device_id=dev, device_id_type=MESH)
                for i, ref in enumerate((rinv_all, obs_all))]

    def mixed(off, rows, src):
        return dot(av[pl.ds(off, rows), :], hb[src]).astype(BF16)

    def layer_rows(l, off, rows, src, put):
        for s in range(loc_members + 1):
            if s < loc_members:
                pre = dot(mb[0:rows, s * nv:(s + 1) * nv], wv[l])
            if s >= 1:
                k = s - 1
                put(k, h[k, pl.ds(off, rows), :] + dot(hid[k % 2, 0:rows, :], uv[l]))
            if s < loc_members:
                hid[s % 2, 0:rows, :] = gelu_of_half(pre).astype(BF16)

    def gather_columns(t):
        for r in range(0, cols, CHUNK):
            macc[r:r + CHUNK, :] += dot(av[r:r + CHUNK, span(t)], hb[0, span(t), :])

    def full_layer(l, c):
        src = l % 2
        if l == 0:
            for r in range(0, cols, CHUNK):
                rest = dot(av[r:r + CHUNK, cols - CHUNK:cols], hb[0, cols - CHUNK:cols, :])
                mb[r:r + CHUNK, :] = (macc[r:r + CHUNK, :] + rest).astype(BF16)
        else:
            mb[...] = mixed(0, cols, src)

        def put(k, new):
            h[k] = new
            hb[1 - src, :, k * nv:(k + 1) * nv] = new.astype(BF16)
        layer_rows(l, 0, cols, src, put)

    def last_layer(t, b):
        l = n_layers - 1
        off = pl.multiple_of(t * CHUNK + b * BLK, BLK)
        mb[0:BLK, :] = mixed(off, BLK, l % 2)

        def put(k, new):
            ht[t, b, k * nv:(k + 1) * nv, :] = new.T
        layer_rows(l, off, BLK, l % 2, put)

    def stats(c, t, b):
        ho = [[ht[t, b, pl.ds(k * nv + obs_i[p], 1), :] for k in range(loc_members)] for p in range(OBS)]
        mo = [sum(x[1:], x[0]) * (1.0 / loc_members) for x in ho]
        y = [[x - mo[p] for x in ho[p]] for p in range(OBS)]
        for p in range(OBS):
            part[c, t, b, ROWS_O + p:ROWS_O + p + 1, :] = mo[p]
        for v in range(0, nv, VB):
            x = [ht[t, b, k * nv + v:k * nv + v + VB, :] for k in range(loc_members)]
            m = sum(x[1:], x[0]) * (1.0 / loc_members)
            d = [z - m for z in x]
            part[c, t, b, v:v + VB, :] = m
            for p in range(OBS):
                o = (p + 1) * BLK + v
                part[c, t, b, o:o + VB, :] = sum(y[p][k] * d[k] for k in range(loc_members))

    def merge(dst, one, two, two_o, half_n, keep):
        for p in range(OBS):
            r = ROWS_O + p
            dst[r:r + 1, :] = 0.5 * (one[r:r + 1, :] + two_o[p])
        sc = [half_n * (two_o[p] - one[ROWS_O + p:ROWS_O + p + 1, :]) for p in range(OBS)]
        for v in range(0, nv, VB):
            ma, mbb = one[v:v + VB, :], two[v:v + VB, :]
            dst[v:v + VB, :] = 0.5 * (ma + mbb)
            dm = mbb - ma
            for p in range(OBS):
                o = (p + 1) * BLK + v
                val = one[o:o + VB, :] + two[o:o + VB, :] + sc[p] * dm
                dst[o:o + VB, :] = val
                if keep:
                    arow[o - BLK:o - BLK + VB, :] = val
        if keep:
            for n, (p, q) in enumerate(PAIRS):
                dst[ROWS_C + n:ROWS_C + n + 1, :] = arow[pl.ds(p * BLK + obs_i[q], 1), :]

    def sib_copy(c, t):
        return pltpu.make_async_remote_copy(
            src_ref=part.at[c, t, 1 - core], dst_ref=got_sib.at[c, t], send_sem=sib_send.at[c, t], recv_sem=sib_recv.at[c, t],
            device_id={'ens': sib}, device_id_type=MESH)

    def chip_copy(c, t):
        return pltpu.make_async_remote_copy(
            src_ref=chip.at[c, t, 0:ROWS_O], dst_ref=got_chip.at[c, t], send_sem=chip_send.at[c, t], recv_sem=chip_recv.at[c, t],
            device_id={'ens': mate}, device_id_type=MESH)

    def tot_copy(c, t):
        return pltpu.make_async_remote_copy(
            src_ref=tot.at[c, t, core], dst_ref=tot.at[c, t, core], send_sem=tot_send.at[c, t], recv_sem=tot_recv.at[c, t],
            device_id={'ens': sib}, device_id_type=MESH)

    def first_merge(c, t):
        sib_copy(c, t).wait_recv()
        two = got_sib.at[c, t]
        two_o = [two[ROWS_O + p:ROWS_O + p + 1, :] for p in range(OBS)]
        merge(chip.at[c, t], part.at[c, t, core], two, two_o, loc_members / 2, False)
        chip_copy(c, t).start()

    def second_merge(c, t):
        chip_copy(c, t).wait_recv()
        two = got_chip.at[c, t]
        mrow[...] = two[0:BLK, :]
        two_o = [mrow[pl.ds(obs_i[p], 1), :] for p in range(OBS)]
        merge(tot.at[c, t, core], chip.at[c, t], two, two_o, loc_members, True)
        tot_copy(c, t).start()

    def update(c, t, b):
        lanes = pl.ds(pl.multiple_of(b * BLK, BLK), BLK)
        rows = pl.ds(pl.multiple_of(t * CHUNK + b * BLK, BLK), BLK)

        def row(r):
            return tot[c, t, b, r:r + 1, :]

        cov = {pq: row(ROWS_C + n) for n, pq in enumerate(PAIRS)}
        rinv = [rinv_all[t, p:p + 1, lanes] for p in range(OBS)]
        innov = [obs_all[t, c, p:p + 1, lanes] - row(ROWS_O + p) for p in range(OBS)]
        ca, cg, ce = ns_weights(cov, rinv, innov, infl_ref[0], members)
        for k in range(loc_members):
            for p in range(OBS):
                yrow[k * OBS + p] = ht[t, b, pl.ds(k * nv + obs_i[p], 1), :] - row(ROWS_O + p)
        for v in range(0, nv, VB):
            m = tot[c, t, b, v:v + VB, :]
            mom = [tot[c, t, b, (p + 1) * BLK + v:(p + 1) * BLK + v + VB, :] for p in range(OBS)]
            base = m + sum(ce[p] * mom[p] for p in range(OBS))
            mix = [sum(cg[sym(p, q)] * mom[q] for q in range(OBS)) for p in range(OBS)]
            for k in range(loc_members):
                r = k * nv + v
                new = base + ca * (ht[t, b, r:r + VB, :] - m)
                for p in range(OBS):
                    new = new + yrow[k * OBS + p] * mix[p]
                ht[t, b, r:r + VB, :] = new
        for k in range(loc_members):
            blk = ht[t, b, k * nv:(k + 1) * nv, :].T
            h[k, rows, :] = blk
            if c < n_cycles - 1:
                hb[0, rows, k * nv:(k + 1) * nv] = blk.astype(BF16)

    def enter(t):
        load_x(t).wait()
        for k in range(loc_members):
            hb[0, span(t), k * nv:(k + 1) * nv] = h[k, span(t), :].astype(BF16)

    macc[...] = jnp.zeros_like(macc)
    loads[0].wait()
    for t in range(2, n_chunks):
        load_x(t).start()
    for load in loads[1:]:
        load.start()

    def begin(t, _):
        enter(t)
        gather_columns(t)
        return 0
    lax.fori_loop(0, n_chunks - 1, begin, 0)
    enter(n_chunks - 1)
    loads[1].wait()
    wv[...] = wv[...] * jnp.bfloat16(0.5)
    loads[2].wait()

    for c in range(n_cycles):
        for l in range(n_layers - 1):
            full_layer(l, c)
            if c == 0 and l == 0:
                for load in loads[3:]:
                    load.wait()
                pl.semaphore_wait(barrier, n_dev - 1)
                for step in range(1, n_dev):
                    for copy in obs_copies(step):
                        copy.start()

        def last(t, _, c=c):
            last_layer(t, 1 - core)
            stats(c, t, 1 - core)
            sib_copy(c, t).start()
            last_layer(t, core)
            stats(c, t, core)
            first_merge(c, t)
            return 0
        lax.fori_loop(0, n_chunks, last, 0)

        if c == 0:
            for step in range(1, n_dev):
                for copy in obs_copies(step):
                    copy.wait()
        if c < n_cycles - 1:
            macc[...] = jnp.zeros_like(macc)

        def finish(t, _, c=c):
            second_merge(c, t)
            update(c, t, core)
            tot_copy(c, t).wait_recv()
            update(c, t, 1 - core)
            if c < n_cycles - 1:
                pl.when(t < n_chunks - 1)(lambda: gather_columns(t))
            return 0
        lax.fori_loop(0, n_chunks, finish, 0)

        def drain(t, _, c=c):
            sib_copy(c, t).wait_send()
            chip_copy(c, t).wait_send()
            tot_copy(c, t).wait_send()
            return 0
        lax.fori_loop(0, n_chunks, drain, 0)


def solution(mesh):
    n_dev = mesh.shape['ens']

    def per_device(x_loc, col_mix, w_in, w_out, obs_loc, rinv_loc, obs_idx, inflation):
        loc, cols, nv = x_loc.shape
        layers, _, ff = w_in.shape
        cycles = obs_loc.shape[0]
        n_chunks = cols // CHUNK
        rinv_t = rinv_loc.T
        obs_t = jnp.swapaxes(obs_loc, 1, 2)
        vm = pl.BlockSpec(memory_space=pltpu.VMEM)
        sm = pl.BlockSpec(memory_space=pltpu.SMEM)
        dma = pltpu.SemaphoreType.DMA
        f32 = jnp.float32
        return pl.pallas_call(
            functools.partial(kernel, n_dev, cycles, loc * n_dev),
            out_shape=pltpu.VMEM(x_loc.shape, x_loc.dtype),
            in_specs=[pl.BlockSpec(memory_space=pltpu.HBM)] * 6 + [sm] * 2,
            out_specs=vm,
            scratch_shapes=[
                pltpu.VMEM((cols, cols), BF16),
                pltpu.VMEM((layers, nv, ff), BF16),
                pltpu.VMEM((layers, ff, nv), BF16),
                pltpu.VMEM((2, cols, loc * nv), BF16),
                pltpu.VMEM((n_chunks, 2, loc * nv, BLK), f32),
                pltpu.VMEM((cols, loc * nv), BF16),
                pltpu.VMEM((2, cols, ff), BF16),
                pltpu.VMEM((cols, loc * nv), f32),
                pltpu.VMEM((n_dev,) + rinv_t.shape, f32),
                pltpu.VMEM((n_dev,) + obs_t.shape, f32),
                pltpu.VMEM((cycles, n_chunks, 2, PART, BLK), f32),
                pltpu.VMEM((cycles, n_chunks, PART, BLK), f32),
                pltpu.VMEM((cycles, n_chunks, PART, BLK), f32),
                pltpu.VMEM((cycles, n_chunks, ROWS_O, BLK), f32),
                pltpu.VMEM((cycles, n_chunks, 2, TOTAL, BLK), f32),
                pltpu.VMEM((BLK, BLK), f32),
                pltpu.VMEM((OBS * BLK, BLK), f32),
                pltpu.VMEM((loc * OBS, 1, BLK), f32),
                dma((n_chunks + 5,)),
                dma((n_dev - 1, 2)), dma((n_dev - 1, 2)),
                dma((cycles, n_chunks)), dma((cycles, n_chunks)),
                dma((cycles, n_chunks)), dma((cycles, n_chunks)),
                dma((cycles, n_chunks)), dma((cycles, n_chunks)),
            ],
            compiler_params=pltpu.CompilerParams(collective_id=0, has_side_effects=True, vmem_limit_bytes=58 * 1024 * 1024),
        )(x_loc, col_mix, w_in, w_out, rinv_t, obs_t, obs_idx, inflation)

    state_spec = P(('case', 'ens'), None, None)
    in_specs = (state_spec, P(), P(), P(), P(None, ('case', 'ens'), None), P(('case', 'ens'), None), P(), P())
    return jax.shard_map(per_device, mesh=mesh, in_specs=in_specs, out_specs=state_spec, check_vma=False)
```

```python
import functools
import math
import jax
import jax.numpy as jnp
from jax import lax
from jax.experimental import pallas as pl
from jax.experimental.pallas import tpu as pltpu
from jax.sharding import PartitionSpec as P

NS_STEPS = 12
OBS = 4
PAIRS = [(p, q) for p in range(OBS) for q in range(p, OBS)]


def sym(p, q):
    return (p, q) if p <= q else (q, p)


def smul(a, b):
    return {(p, q): sum(a[sym(p, t)] * b[sym(t, q)] for t in range(OBS)) for p, q in PAIRS}


def shift(c, a):
    return {pq: (v + c if pq[0] == pq[1] else v) for pq, v in a.items()}


def ns_weights(cov, rinv, innov, inflation, members):
    root_r = [jnp.sqrt(r) for r in rinv]
    base = (members - 1) / inflation
    b_hat = shift(base, {(p, q): cov[(p, q)] * root_r[p] * root_r[q] for p, q in PAIRS})
    norm2 = (members - OBS) * base * base
    for (p, q), v in b_hat.items():
        norm2 = norm2 + (v * v if p == q else 2.0 * (v * v))
    norm = jnp.sqrt(norm2)
    inv = 1.0 / norm
    full = (8, inv.shape[1])
    sub = lax.broadcasted_iota(jnp.int32, full, 0)

    def spread(x):
        return jnp.broadcast_to(x, full)

    state = {}
    for p, q in PAIRS:
        rest = jnp.where(sub == 1, spread(inv), jnp.where(sub == 2, 1.0, 0.0)) if p == q else jnp.zeros(full, jnp.float32)
        state[(p, q)] = jnp.where(sub == 0, spread(b_hat[(p, q)] * inv), rest)
    coef = jnp.where(sub == 1, spread(base * inv), jnp.where(sub == 3, 1.0, 0.0))
    for step in range(NS_STEPS):
        tau = 1.5 - 0.5 * spread(coef[1:2])
        t_hat = shift(1.5, {pq: -0.5 * spread(v[0:1]) for pq, v in state.items()})
        t_low = {pq: -0.5 * spread(v[1:2]) for pq, v in state.items()}
        prod = smul(state, t_hat)
        state = {pq: prod[pq] + coef * t_low[pq] for pq in PAIRS}
        coef = coef * tau
        if step < NS_STEPS - 1:
            prod = smul(state, t_hat)
            state = {pq: jnp.where(sub < 2, prod[pq] + coef * t_low[pq], state[pq]) for pq in PAIRS}
            coef = jnp.where(sub < 2, coef * tau, coef)
    inv_root = 1.0 / jnp.sqrt(norm)
    s_hat = {pq: v[2:3] * inv_root for pq, v in state.items()}
    q_mat = {pq: v[3:4] * inv_root for pq, v in state.items()}
    vec = [root_r[p] * innov[p] for p in range(OBS)]
    for _ in range(2):
        vec = [sum(s_hat[sym(p, q)] * vec[q] for q in range(OBS)) for p in range(OBS)]
    fac = math.sqrt(members - 1)
    a = fac * (coef[3:4] * inv_root)
    g = {(p, q): fac * root_r[p] * root_r[q] * q_mat[(p, q)] for p, q in PAIRS}
    e = [root_r[p] * vec[p] for p in range(OBS)]
    return a, g, e


MESH = pl.DeviceIdType.MESH
CHUNK = 256
BLK = 128
ROWS_O = 5 * BLK
PART = ROWS_O + 8
VB = 16
BF16 = jnp.bfloat16


def dot(a, b):
    return jnp.dot(a, b, preferred_element_type=jnp.float32)


def gelu_of_half(z):
    return z + z * jnp.tanh(z * (2 * 0.7978845608028654 + (8 * 0.035677408136300125) * (z * z)))


def kernel(n_dev, n_cycles, members, x_hbm, a_hbm, w_hbm, u_hbm, rinv_hbm, obs_hbm, idx_ref, infl_ref, h,
           av, wv, uv, hb, ht, mb, hid, macc, rinv_all, obs_all, part, got_sib, chip, got_chip, tot, totrow, mrow, arow, yrow,
           load_sem, obs_send, obs_recv, sib_send, sib_recv, chip_send, chip_recv, tot_send, tot_recv, row_send, row_recv):
    loc_members, cols, nv = h.shape
    n_layers = wv.shape[0]
    n_chunks = cols // CHUNK
    me = lax.axis_index('ens')
    core = lax.rem(me, 2)
    sib = me + 1 - 2 * core
    mate = lax.rem(me + 2, n_dev)
    obs_i = [idx_ref[p] for p in range(OBS)]

    def span(t):
        return pl.ds(pl.multiple_of(t * CHUNK, CHUNK), CHUNK)

    def load_x(t):
        return pltpu.make_async_copy(x_hbm.at[:, span(t), :], h.at[:, span(t), :], load_sem.at[t])

    loads = [pltpu.make_async_copy(src, dst, load_sem.at[n_chunks + i]) for i, (src, dst) in enumerate(
        ((a_hbm, av), (w_hbm, wv), (u_hbm, uv), (rinv_hbm, rinv_all.at[me]), (obs_hbm, obs_all.at[me])))]
    loads[0].start()
    load_x(0).start()
    load_x(1).start()

    barrier = pltpu.get_barrier_semaphore()
    for step in range(1, n_dev):
        pl.semaphore_signal(barrier, inc=1, device_id={'ens': lax.rem(me + step, n_dev)}, device_id_type=MESH)

    def obs_copies(step):
        dev = {'ens': lax.rem(me + step, n_dev)}
        return [pltpu.make_async_remote_copy(src_ref=ref.at[me], dst_ref=ref.at[me], send_sem=obs_send.at[step - 1, i],
                                             recv_sem=obs_recv.at[step - 1, i], device_id=dev, device_id_type=MESH)
                for i, ref in enumerate((rinv_all, obs_all))]

    def mixed(off, rows, src):
        return dot(av[pl.ds(off, rows), :], hb[src]).astype(BF16)

    def layer_rows(l, off, rows, src, put):
        for s in range(loc_members + 1):
            if s < loc_members:
                pre = dot(mb[0:rows, s * nv:(s + 1) * nv], wv[l])
            if s >= 1:
                k = s - 1
                put(k, h[k, pl.ds(off, rows), :] + dot(hid[k % 2, 0:rows, :], uv[l]))
            if s < loc_members:
                hid[s % 2, 0:rows, :] = gelu_of_half(pre).astype(BF16)

    def gather_columns(t):
        for r in range(0, cols, CHUNK):
            macc[r:r + CHUNK, :] += dot(av[r:r + CHUNK, span(t)], hb[0, span(t), :])

    def full_layer(l, c):
        src = l % 2
        if l == 0:
            for r in range(0, cols, CHUNK):
                rest = dot(av[r:r + CHUNK, cols - CHUNK:cols], hb[0, cols - CHUNK:cols, :])
                mb[r:r + CHUNK, :] = (macc[r:r + CHUNK, :] + rest).astype(BF16)
        else:
            mb[...] = mixed(0, cols, src)

        def put(k, new):
            h[k] = new
            hb[1 - src, :, k * nv:(k + 1) * nv] = new.astype(BF16)
        layer_rows(l, 0, cols, src, put)

    def last_layer(t, b):
        l = n_layers - 1
        off = pl.multiple_of(t * CHUNK + b * BLK, BLK)
        mb[0:BLK, :] = mixed(off, BLK, l % 2)

        def put(k, new):
            ht[t, b, k * nv:(k + 1) * nv, :] = new.T
        layer_rows(l, off, BLK, l % 2, put)

    def stats(c, t, b):
        ho = [[ht[t, b, pl.ds(k * nv + obs_i[p], 1), :] for k in range(loc_members)] for p in range(OBS)]
        mo = [sum(x[1:], x[0]) * (1.0 / loc_members) for x in ho]
        y = [[x - mo[p] for x in ho[p]] for p in range(OBS)]
        for p in range(OBS):
            part[c, t, b, ROWS_O + p:ROWS_O + p + 1, :] = mo[p]
        for v in range(0, nv, VB):
            x = [ht[t, b, k * nv + v:k * nv + v + VB, :] for k in range(loc_members)]
            m = sum(x[1:], x[0]) * (1.0 / loc_members)
            d = [z - m for z in x]
            part[c, t, b, v:v + VB, :] = m
            for p in range(OBS):
                o = (p + 1) * BLK + v
                part[c, t, b, o:o + VB, :] = sum(y[p][k] * d[k] for k in range(loc_members))

    def merge(dst, dst_o, one, two, two_o, half_n, keep):
        for p in range(OBS):
            dst_o[p:p + 1, :] = 0.5 * (one[ROWS_O + p:ROWS_O + p + 1, :] + two_o[p])
        sc = [half_n * (two_o[p] - one[ROWS_O + p:ROWS_O + p + 1, :]) for p in range(OBS)]
        for v in range(0, nv, VB):
            ma, mbb = one[v:v + VB, :], two[v:v + VB, :]
            dst[v:v + VB, :] = 0.5 * (ma + mbb)
            dm = mbb - ma
            for p in range(OBS):
                o = (p + 1) * BLK + v
                val = one[o:o + VB, :] + two[o:o + VB, :] + sc[p] * dm
                dst[o:o + VB, :] = val
                if keep:
                    arow[o - BLK:o - BLK + VB, :] = val
    def sib_copy(c, t):
        return pltpu.make_async_remote_copy(
            src_ref=part.at[c, t, 1 - core], dst_ref=got_sib.at[c, t], send_sem=sib_send.at[c, t], recv_sem=sib_recv.at[c, t],
            device_id={'ens': sib}, device_id_type=MESH)

    def chip_copy(c, t):
        return pltpu.make_async_remote_copy(
            src_ref=chip.at[c, t, 0:ROWS_O], dst_ref=got_chip.at[c, t], send_sem=chip_send.at[c, t], recv_sem=chip_recv.at[c, t],
            device_id={'ens': mate}, device_id_type=MESH)

    def tot_copy(c, t):
        return pltpu.make_async_remote_copy(
            src_ref=tot.at[c, t, core], dst_ref=tot.at[c, t, core], send_sem=tot_send.at[c, t], recv_sem=tot_recv.at[c, t],
            device_id={'ens': sib}, device_id_type=MESH)

    def row_copy(c, t):
        return pltpu.make_async_remote_copy(
            src_ref=totrow.at[c, t, core], dst_ref=totrow.at[c, t, core], send_sem=row_send.at[c, t], recv_sem=row_recv.at[c, t],
            device_id={'ens': sib}, device_id_type=MESH)

    def first_merge(c, t):
        sib_copy(c, t).wait_recv()
        two = got_sib.at[c, t]
        two_o = [two[ROWS_O + p:ROWS_O + p + 1, :] for p in range(OBS)]
        merge(chip.at[c, t], chip.at[c, t, ROWS_O:PART], part.at[c, t, core], two, two_o, loc_members / 2, False)
        chip_copy(c, t).start()

    def second_merge(c, t):
        chip_copy(c, t).wait_recv()
        two = got_chip.at[c, t]
        mrow[...] = two[0:BLK, :]
        two_o = [mrow[pl.ds(obs_i[p], 1), :] for p in range(OBS)]
        merge(tot.at[c, t, core], totrow.at[c, t, core], chip.at[c, t], two, two_o, loc_members, True)
        for n, (p, q) in enumerate(PAIRS):
            totrow[c, t, core, OBS + n:OBS + n + 1, :] = arow[pl.ds(p * BLK + obs_i[q], 1), :]
        row_copy(c, t).start()
        tot_copy(c, t).start()

    def weights(c, t, b):
        lanes = pl.ds(pl.multiple_of(b * BLK, BLK), BLK)

        def row(r):
            return totrow[c, t, b, r:r + 1, :]

        cov = {pq: row(OBS + n) for n, pq in enumerate(PAIRS)}
        rinv = [rinv_all[t, p:p + 1, lanes] for p in range(OBS)]
        innov = [obs_all[t, c, p:p + 1, lanes] - row(p) for p in range(OBS)]
        for k in range(loc_members):
            for p in range(OBS):
                yrow[k * OBS + p] = ht[t, b, pl.ds(k * nv + obs_i[p], 1), :] - row(p)
        return ns_weights(cov, rinv, innov, infl_ref[0], members)

    def apply(c, t, b, ca, cg, ce):
        rows = pl.ds(pl.multiple_of(t * CHUNK + b * BLK, BLK), BLK)
        for v in range(0, nv, VB):
            m = tot[c, t, b, v:v + VB, :]
            mom = [tot[c, t, b, (p + 1) * BLK + v:(p + 1) * BLK + v + VB, :] for p in range(OBS)]
            base = m + sum(ce[p] * mom[p] for p in range(OBS))
            mix = [sum(cg[sym(p, q)] * mom[q] for q in range(OBS)) for p in range(OBS)]
            for k in range(loc_members):
                r = k * nv + v
                new = base + ca * (ht[t, b, r:r + VB, :] - m)
                for p in range(OBS):
                    new = new + yrow[k * OBS + p] * mix[p]
                ht[t, b, r:r + VB, :] = new
        for k in range(loc_members):
            blk = ht[t, b, k * nv:(k + 1) * nv, :].T
            h[k, rows, :] = blk
            if c < n_cycles - 1:
                hb[0, rows, k * nv:(k + 1) * nv] = blk.astype(BF16)

    def enter(t):
        load_x(t).wait()
        for k in range(loc_members):
            hb[0, span(t), k * nv:(k + 1) * nv] = h[k, span(t), :].astype(BF16)

    macc[...] = jnp.zeros_like(macc)
    loads[0].wait()
    for t in range(2, n_chunks):
        load_x(t).start()
    for load in loads[1:]:
        load.start()

    def begin(t, _):
        enter(t)
        gather_columns(t)
        return 0
    lax.fori_loop(0, n_chunks - 1, begin, 0)
    enter(n_chunks - 1)
    loads[1].wait()
    wv[...] = wv[...] * jnp.bfloat16(0.5)
    loads[2].wait()

    for c in range(n_cycles):
        for l in range(n_layers - 1):
            full_layer(l, c)
            if c == 0 and l == 0:
                for load in loads[3:]:
                    load.wait()
                pl.semaphore_wait(barrier, n_dev - 1)
                for step in range(1, n_dev):
                    for copy in obs_copies(step):
                        copy.start()

        def last(t, _, c=c):
            last_layer(t, 1 - core)
            stats(c, t, 1 - core)
            sib_copy(c, t).start()
            last_layer(t, core)
            stats(c, t, core)
            first_merge(c, t)
            return 0
        lax.fori_loop(0, n_chunks, last, 0)

        if c == 0:
            for step in range(1, n_dev):
                for copy in obs_copies(step):
                    copy.wait()
        if c < n_cycles - 1:
            macc[...] = jnp.zeros_like(macc)

        def finish(t, _, c=c):
            sib_copy(c, t).wait_send()
            second_merge(c, t)
            apply(c, t, core, *weights(c, t, core))
            chip_copy(c, t).wait_send()
            row_copy(c, t).wait_recv()
            other = weights(c, t, 1 - core)
            tot_copy(c, t).wait_recv()
            apply(c, t, 1 - core, *other)
            if c < n_cycles - 1:
                pl.when(t < n_chunks - 1)(lambda: gather_columns(t))
            tot_copy(c, t).wait_send()
            row_copy(c, t).wait_send()
            return 0
        lax.fori_loop(0, n_chunks, finish, 0)


def solution(mesh):
    n_dev = mesh.shape['ens']

    def per_device(x_loc, col_mix, w_in, w_out, obs_loc, rinv_loc, obs_idx, inflation):
        loc, cols, nv = x_loc.shape
        layers, _, ff = w_in.shape
        cycles = obs_loc.shape[0]
        n_chunks = cols // CHUNK
        rinv_t = rinv_loc.T
        obs_t = jnp.swapaxes(obs_loc, 1, 2)
        vm = pl.BlockSpec(memory_space=pltpu.VMEM)
        sm = pl.BlockSpec(memory_space=pltpu.SMEM)
        dma = pltpu.SemaphoreType.DMA
        f32 = jnp.float32
        return pl.pallas_call(
            functools.partial(kernel, n_dev, cycles, loc * n_dev),
            out_shape=pltpu.VMEM(x_loc.shape, x_loc.dtype),
            in_specs=[pl.BlockSpec(memory_space=pltpu.HBM)] * 6 + [sm] * 2,
            out_specs=vm,
            scratch_shapes=[
                pltpu.VMEM((cols, cols), BF16),
                pltpu.VMEM((layers, nv, ff), BF16),
                pltpu.VMEM((layers, ff, nv), BF16),
                pltpu.VMEM((2, cols, loc * nv), BF16),
                pltpu.VMEM((n_chunks, 2, loc * nv, BLK), f32),
                pltpu.VMEM((cols, loc * nv), BF16),
                pltpu.VMEM((2, cols, ff), BF16),
                pltpu.VMEM((cols, loc * nv), f32),
                pltpu.VMEM((n_dev,) + rinv_t.shape, f32),
                pltpu.VMEM((n_dev,) + obs_t.shape, f32),
                pltpu.VMEM((cycles, n_chunks, 2, PART, BLK), f32),
                pltpu.VMEM((cycles, n_chunks, PART, BLK), f32),
                pltpu.VMEM((cycles, n_chunks, PART, BLK), f32),
                pltpu.VMEM((cycles, n_chunks, ROWS_O, BLK), f32),
                pltpu.VMEM((cycles, n_chunks, 2, ROWS_O, BLK), f32),
                pltpu.VMEM((cycles, n_chunks, 2, 16, BLK), f32),
                pltpu.VMEM((BLK, BLK), f32),
                pltpu.VMEM((OBS * BLK, BLK), f32),
                pltpu.VMEM((loc * OBS, 1, BLK), f32),
                dma((n_chunks + 5,)),
                dma((n_dev - 1, 2)), dma((n_dev - 1, 2)),
                dma((cycles, n_chunks)), dma((cycles, n_chunks)),
                dma((cycles, n_chunks)), dma((cycles, n_chunks)),
                dma((cycles, n_chunks)), dma((cycles, n_chunks)),
                dma((cycles, n_chunks)), dma((cycles, n_chunks)),
            ],
            compiler_params=pltpu.CompilerParams(collective_id=0, has_side_effects=True, vmem_limit_bytes=58 * 1024 * 1024),
        )(x_loc, col_mix, w_in, w_out, rinv_t, obs_t, obs_idx, inflation)

    state_spec = P(('case', 'ens'), None, None)
    in_specs = (state_spec, P(), P(), P(), P(None, ('case', 'ens'), None), P(('case', 'ens'), None), P(), P())
    return jax.shard_map(per_device, mesh=mesh, in_specs=in_specs, out_specs=state_spec, check_vma=False)
```

```python
import functools
import math
import jax
import jax.numpy as jnp
from jax import lax
from jax.experimental import pallas as pl
from jax.experimental.pallas import tpu as pltpu
from jax.sharding import PartitionSpec as P

NS_STEPS = 12
OBS = 4
PAIRS = [(p, q) for p in range(OBS) for q in range(p, OBS)]


def sym(p, q):
    return (p, q) if p <= q else (q, p)


def smul(a, b):
    return {(p, q): sum(a[sym(p, t)] * b[sym(t, q)] for t in range(OBS)) for p, q in PAIRS}


def shift(c, a):
    return {pq: (v + c if pq[0] == pq[1] else v) for pq, v in a.items()}


def ns_weights(cov, rinv, innov, inflation, members):
    root_r = [jnp.sqrt(r) for r in rinv]
    base = (members - 1) / inflation
    b_hat = shift(base, {(p, q): cov[(p, q)] * root_r[p] * root_r[q] for p, q in PAIRS})
    norm2 = (members - OBS) * base * base
    for (p, q), v in b_hat.items():
        norm2 = norm2 + (v * v if p == q else 2.0 * (v * v))
    norm = jnp.sqrt(norm2)
    inv = 1.0 / norm
    full = (8, inv.shape[1])
    sub = lax.broadcasted_iota(jnp.int32, full, 0)

    def spread(x):
        return jnp.broadcast_to(x, full)

    state = {}
    for p, q in PAIRS:
        rest = jnp.where(sub == 1, spread(inv), jnp.where(sub == 2, 1.0, 0.0)) if p == q else jnp.zeros(full, jnp.float32)
        state[(p, q)] = jnp.where(sub == 0, spread(b_hat[(p, q)] * inv), rest)
    coef = jnp.where(sub == 1, spread(base * inv), jnp.where(sub == 3, 1.0, 0.0))
    for step in range(NS_STEPS):
        tau = 1.5 - 0.5 * spread(coef[1:2])
        t_hat = shift(1.5, {pq: -0.5 * spread(v[0:1]) for pq, v in state.items()})
        t_low = {pq: -0.5 * spread(v[1:2]) for pq, v in state.items()}
        prod = smul(state, t_hat)
        state = {pq: prod[pq] + coef * t_low[pq] for pq in PAIRS}
        coef = coef * tau
        if step < NS_STEPS - 1:
            prod = smul(state, t_hat)
            state = {pq: jnp.where(sub < 2, prod[pq] + coef * t_low[pq], state[pq]) for pq in PAIRS}
            coef = jnp.where(sub < 2, coef * tau, coef)
    inv_root = 1.0 / jnp.sqrt(norm)
    s_hat = {pq: v[2:3] * inv_root for pq, v in state.items()}
    q_mat = {pq: v[3:4] * inv_root for pq, v in state.items()}
    vec = [root_r[p] * innov[p] for p in range(OBS)]
    for _ in range(2):
        vec = [sum(s_hat[sym(p, q)] * vec[q] for q in range(OBS)) for p in range(OBS)]
    fac = math.sqrt(members - 1)
    a = fac * (coef[3:4] * inv_root)
    g = {(p, q): fac * root_r[p] * root_r[q] * q_mat[(p, q)] for p, q in PAIRS}
    e = [root_r[p] * vec[p] for p in range(OBS)]
    return a, g, e


MESH = pl.DeviceIdType.MESH
CHUNK = 256
BLK = 128
ROWS_O = 5 * BLK
PART = ROWS_O + 8
VB = 16
BF16 = jnp.bfloat16


def dot(a, b):
    return jnp.dot(a, b, preferred_element_type=jnp.float32)


def gelu_of_half(z):
    return z + z * jnp.tanh(z * (2 * 0.7978845608028654 + (8 * 0.035677408136300125) * (z * z)))


def kernel(n_dev, n_cycles, members, x_hbm, a_hbm, w_hbm, u_hbm, rinv_hbm, obs_hbm, idx_ref, infl_ref, h,
           av, wv, uv, hb, ht, mb, hid, macc, rinv_all, obs_all, part, got_sib, chip, got_chip, tot, totrow, mrow, arow, yrow,
           load_sem, rest_sem, obs_send, obs_recv, sib_send, sib_recv, chip_send, chip_recv, tot_send, tot_recv, row_send, row_recv):
    loc_members, cols, nv = h.shape
    n_layers = wv.shape[0]
    n_chunks = cols // CHUNK
    me = lax.axis_index('ens')
    core = lax.rem(me, 2)
    sib = me + 1 - 2 * core
    mate = lax.rem(me + 2, n_dev)
    obs_i = [idx_ref[p] for p in range(OBS)]

    def span(t):
        return pl.ds(pl.multiple_of(t * CHUNK, CHUNK), CHUNK)

    def load_piece(t):
        return (pltpu.make_async_copy(x_hbm.at[:, span(t), :], h.at[:, span(t), :], load_sem.at[t, 0]),
                pltpu.make_async_copy(a_hbm.at[:, span(t)], av.at[:, span(t)], load_sem.at[t, 1]))

    def start_piece(t):
        for load in load_piece(t):
            load.start()

    loads = [pltpu.make_async_copy(src, dst, rest_sem.at[i]) for i, (src, dst) in enumerate(
        ((w_hbm, wv), (u_hbm, uv), (rinv_hbm, rinv_all.at[me]), (obs_hbm, obs_all.at[me])))]
    start_piece(0)
    start_piece(1)
    start_piece(2)

    barrier = pltpu.get_barrier_semaphore()
    for step in range(1, n_dev):
        pl.semaphore_signal(barrier, inc=1, device_id={'ens': lax.rem(me + step, n_dev)}, device_id_type=MESH)

    def obs_copies(step):
        dev = {'ens': lax.rem(me + step, n_dev)}
        return [pltpu.make_async_remote_copy(src_ref=ref.at[me], dst_ref=ref.at[me], send_sem=obs_send.at[step - 1, i],
                                             recv_sem=obs_recv.at[step - 1, i], device_id=dev, device_id_type=MESH)
                for i, ref in enumerate((rinv_all, obs_all))]

    def mixed(off, rows, src):
        return dot(av[pl.ds(off, rows), :], hb[src]).astype(BF16)

    def layer_rows(l, off, rows, src, put):
        for s in range(loc_members + 1):
            if s < loc_members:
                pre = dot(mb[0:rows, s * nv:(s + 1) * nv], wv[l])
            if s >= 1:
                k = s - 1
                put(k, h[k, pl.ds(off, rows), :] + dot(hid[k % 2, 0:rows, :], uv[l]))
            if s < loc_members:
                hid[s % 2, 0:rows, :] = gelu_of_half(pre).astype(BF16)

    def gather_columns(t):
        for r in range(0, cols, CHUNK):
            macc[r:r + CHUNK, :] += dot(av[r:r + CHUNK, span(t)], hb[0, span(t), :])

    def full_layer(l, c):
        src = l % 2
        if l == 0:
            for r in range(0, cols, CHUNK):
                rest = dot(av[r:r + CHUNK, cols - CHUNK:cols], hb[0, cols - CHUNK:cols, :])
                mb[r:r + CHUNK, :] = (macc[r:r + CHUNK, :] + rest).astype(BF16)
        else:
            mb[...] = mixed(0, cols, src)

        def put(k, new):
            h[k] = new
            hb[1 - src, :, k * nv:(k + 1) * nv] = new.astype(BF16)
        layer_rows(l, 0, cols, src, put)

    def last_layer(t, b):
        l = n_layers - 1
        off = pl.multiple_of(t * CHUNK + b * BLK, BLK)
        mb[0:BLK, :] = mixed(off, BLK, l % 2)

        def put(k, new):
            ht[t, b, k * nv:(k + 1) * nv, :] = new.T
        layer_rows(l, off, BLK, l % 2, put)

    def stats(c, t, b):
        ho = [[ht[t, b, pl.ds(k * nv + obs_i[p], 1), :] for k in range(loc_members)] for p in range(OBS)]
        mo = [sum(x[1:], x[0]) * (1.0 / loc_members) for x in ho]
        y = [[x - mo[p] for x in ho[p]] for p in range(OBS)]
        for p in range(OBS):
            part[c, t, b, ROWS_O + p:ROWS_O + p + 1, :] = mo[p]
        for v in range(0, nv, VB):
            x = [ht[t, b, k * nv + v:k * nv + v + VB, :] for k in range(loc_members)]
            m = sum(x[1:], x[0]) * (1.0 / loc_members)
            d = [z - m for z in x]
            part[c, t, b, v:v + VB, :] = m
            for p in range(OBS):
                o = (p + 1) * BLK + v
                part[c, t, b, o:o + VB, :] = sum(y[p][k] * d[k] for k in range(loc_members))

    def merge(dst, dst_o, one, two, two_o, half_n, keep):
        for p in range(OBS):
            dst_o[p:p + 1, :] = 0.5 * (one[ROWS_O + p:ROWS_O + p + 1, :] + two_o[p])
        sc = [half_n * (two_o[p] - one[ROWS_O + p:ROWS_O + p + 1, :]) for p in range(OBS)]
        for v in range(0, nv, VB):
            ma, mbb = one[v:v + VB, :], two[v:v + VB, :]
            dst[v:v + VB, :] = 0.5 * (ma + mbb)
            dm = mbb - ma
            for p in range(OBS):
                o = (p + 1) * BLK + v
                val = one[o:o + VB, :] + two[o:o + VB, :] + sc[p] * dm
                dst[o:o + VB, :] = val
                if keep:
                    arow[o - BLK:o - BLK + VB, :] = val
    def sib_copy(c, t):
        return pltpu.make_async_remote_copy(
            src_ref=part.at[c, t, 1 - core], dst_ref=got_sib.at[c, t], send_sem=sib_send.at[c, t], recv_sem=sib_recv.at[c, t],
            device_id={'ens': sib}, device_id_type=MESH)

    def chip_copy(c, t):
        return pltpu.make_async_remote_copy(
            src_ref=chip.at[c, t, 0:ROWS_O], dst_ref=got_chip.at[c, t], send_sem=chip_send.at[c, t], recv_sem=chip_recv.at[c, t],
            device_id={'ens': mate}, device_id_type=MESH)

    def tot_copy(c, t):
        return pltpu.make_async_remote_copy(
            src_ref=tot.at[c, t, core], dst_ref=tot.at[c, t, core], send_sem=tot_send.at[c, t], recv_sem=tot_recv.at[c, t],
            device_id={'ens': sib}, device_id_type=MESH)

    def row_copy(c, t):
        return pltpu.make_async_remote_copy(
            src_ref=totrow.at[c, t, core], dst_ref=totrow.at[c, t, core], send_sem=row_send.at[c, t], recv_sem=row_recv.at[c, t],
            device_id={'ens': sib}, device_id_type=MESH)

    def first_merge(c, t):
        sib_copy(c, t).wait_recv()
        two = got_sib.at[c, t]
        two_o = [two[ROWS_O + p:ROWS_O + p + 1, :] for p in range(OBS)]
        merge(chip.at[c, t], chip.at[c, t, ROWS_O:PART], part.at[c, t, core], two, two_o, loc_members / 2, False)
        chip_copy(c, t).start()

    def second_merge(c, t):
        chip_copy(c, t).wait_recv()
        two = got_chip.at[c, t]
        mrow[...] = two[0:BLK, :]
        two_o = [mrow[pl.ds(obs_i[p], 1), :] for p in range(OBS)]
        merge(tot.at[c, t, core], totrow.at[c, t, core], chip.at[c, t], two, two_o, loc_members, True)
        for n, (p, q) in enumerate(PAIRS):
            totrow[c, t, core, OBS + n:OBS + n + 1, :] = arow[pl.ds(p * BLK + obs_i[q], 1), :]
        row_copy(c, t).start()
        tot_copy(c, t).start()

    def weights(c, t, b):
        lanes = pl.ds(pl.multiple_of(b * BLK, BLK), BLK)

        def row(r):
            return totrow[c, t, b, r:r + 1, :]

        cov = {pq: row(OBS + n) for n, pq in enumerate(PAIRS)}
        rinv = [rinv_all[t, p:p + 1, lanes] for p in range(OBS)]
        innov = [obs_all[t, c, p:p + 1, lanes] - row(p) for p in range(OBS)]
        for k in range(loc_members):
            for p in range(OBS):
                yrow[k * OBS + p] = ht[t, b, pl.ds(k * nv + obs_i[p], 1), :] - row(p)
        return ns_weights(cov, rinv, innov, infl_ref[0], members)

    def apply(c, t, b, ca, cg, ce):
        rows = pl.ds(pl.multiple_of(t * CHUNK + b * BLK, BLK), BLK)
        for v in range(0, nv, VB):
            m = tot[c, t, b, v:v + VB, :]
            mom = [tot[c, t, b, (p + 1) * BLK + v:(p + 1) * BLK + v + VB, :] for p in range(OBS)]
            base = m + sum(ce[p] * mom[p] for p in range(OBS))
            mix = [sum(cg[sym(p, q)] * mom[q] for q in range(OBS)) for p in range(OBS)]
            for k in range(loc_members):
                r = k * nv + v
                new = base + ca * (ht[t, b, r:r + VB, :] - m)
                for p in range(OBS):
                    new = new + yrow[k * OBS + p] * mix[p]
                ht[t, b, r:r + VB, :] = new
        for k in range(loc_members):
            blk = ht[t, b, k * nv:(k + 1) * nv, :].T
            h[k, rows, :] = blk
            if c < n_cycles - 1:
                hb[0, rows, k * nv:(k + 1) * nv] = blk.astype(BF16)

    def enter(t):
        for load in load_piece(t):
            load.wait()
        for k in range(loc_members):
            hb[0, span(t), k * nv:(k + 1) * nv] = h[k, span(t), :].astype(BF16)

    macc[...] = jnp.zeros_like(macc)

    def begin(t, _):
        enter(t)
        pl.when(t + 3 < n_chunks)(lambda: start_piece(t + 3))

        @pl.when(t == 0)
        def _():
            for load in loads:
                load.start()
        gather_columns(t)
        return 0
    lax.fori_loop(0, n_chunks - 1, begin, 0)
    enter(n_chunks - 1)
    loads[0].wait()
    wv[...] = wv[...] * jnp.bfloat16(0.5)
    loads[1].wait()

    for c in range(n_cycles):
        for l in range(n_layers - 1):
            full_layer(l, c)
            if c == 0 and l == 0:
                for load in loads[2:]:
                    load.wait()
                pl.semaphore_wait(barrier, n_dev - 1)
                for step in range(1, n_dev):
                    for copy in obs_copies(step):
                        copy.start()

        def last(t, _, c=c):
            last_layer(t, 1 - core)
            stats(c, t, 1 - core)
            sib_copy(c, t).start()
            last_layer(t, core)
            stats(c, t, core)
            first_merge(c, t)
            return 0
        lax.fori_loop(0, n_chunks, last, 0)

        if c == 0:
            for step in range(1, n_dev):
                for copy in obs_copies(step):
                    copy.wait()
        if c < n_cycles - 1:
            macc[...] = jnp.zeros_like(macc)

        def finish(t, _, c=c):
            sib_copy(c, t).wait_send()
            second_merge(c, t)
            apply(c, t, core, *weights(c, t, core))
            chip_copy(c, t).wait_send()
            row_copy(c, t).wait_recv()
            other = weights(c, t, 1 - core)
            tot_copy(c, t).wait_recv()
            apply(c, t, 1 - core, *other)
            if c < n_cycles - 1:
                pl.when(t < n_chunks - 1)(lambda: gather_columns(t))
            tot_copy(c, t).wait_send()
            row_copy(c, t).wait_send()
            return 0
        lax.fori_loop(0, n_chunks, finish, 0)


def solution(mesh):
    n_dev = mesh.shape['ens']

    def per_device(x_loc, col_mix, w_in, w_out, obs_loc, rinv_loc, obs_idx, inflation):
        loc, cols, nv = x_loc.shape
        layers, _, ff = w_in.shape
        cycles = obs_loc.shape[0]
        n_chunks = cols // CHUNK
        rinv_t = rinv_loc.T
        obs_t = jnp.swapaxes(obs_loc, 1, 2)
        vm = pl.BlockSpec(memory_space=pltpu.VMEM)
        sm = pl.BlockSpec(memory_space=pltpu.SMEM)
        dma = pltpu.SemaphoreType.DMA
        f32 = jnp.float32
        return pl.pallas_call(
            functools.partial(kernel, n_dev, cycles, loc * n_dev),
            out_shape=pltpu.VMEM(x_loc.shape, x_loc.dtype),
            in_specs=[pl.BlockSpec(memory_space=pltpu.HBM)] * 6 + [sm] * 2,
            out_specs=vm,
            scratch_shapes=[
                pltpu.VMEM((cols, cols), BF16),
                pltpu.VMEM((layers, nv, ff), BF16),
                pltpu.VMEM((layers, ff, nv), BF16),
                pltpu.VMEM((2, cols, loc * nv), BF16),
                pltpu.VMEM((n_chunks, 2, loc * nv, BLK), f32),
                pltpu.VMEM((cols, loc * nv), BF16),
                pltpu.VMEM((2, cols, ff), BF16),
                pltpu.VMEM((cols, loc * nv), f32),
                pltpu.VMEM((n_dev,) + rinv_t.shape, f32),
                pltpu.VMEM((n_dev,) + obs_t.shape, f32),
                pltpu.VMEM((cycles, n_chunks, 2, PART, BLK), f32),
                pltpu.VMEM((cycles, n_chunks, PART, BLK), f32),
                pltpu.VMEM((cycles, n_chunks, PART, BLK), f32),
                pltpu.VMEM((cycles, n_chunks, ROWS_O, BLK), f32),
                pltpu.VMEM((cycles, n_chunks, 2, ROWS_O, BLK), f32),
                pltpu.VMEM((cycles, n_chunks, 2, 16, BLK), f32),
                pltpu.VMEM((BLK, BLK), f32),
                pltpu.VMEM((OBS * BLK, BLK), f32),
                pltpu.VMEM((loc * OBS, 1, BLK), f32),
                dma((n_chunks, 2)), dma((4,)),
                dma((n_dev - 1, 2)), dma((n_dev - 1, 2)),
                dma((cycles, n_chunks)), dma((cycles, n_chunks)),
                dma((cycles, n_chunks)), dma((cycles, n_chunks)),
                dma((cycles, n_chunks)), dma((cycles, n_chunks)),
                dma((cycles, n_chunks)), dma((cycles, n_chunks)),
            ],
            compiler_params=pltpu.CompilerParams(collective_id=0, has_side_effects=True, vmem_limit_bytes=58 * 1024 * 1024),
        )(x_loc, col_mix, w_in, w_out, rinv_t, obs_t, obs_idx, inflation)

    state_spec = P(('case', 'ens'), None, None)
    in_specs = (state_spec, P(), P(), P(), P(None, ('case', 'ens'), None), P(('case', 'ens'), None), P(), P())
    return jax.shard_map(per_device, mesh=mesh, in_specs=in_specs, out_specs=state_spec, check_vma=False)
```

```python
import functools
import math
import jax
import jax.numpy as jnp
from jax import lax
from jax.experimental import pallas as pl
from jax.experimental.pallas import tpu as pltpu
from jax.sharding import PartitionSpec as P

NS_STEPS = 12
OBS = 4
PAIRS = [(p, q) for p in range(OBS) for q in range(p, OBS)]


def sym(p, q):
    return (p, q) if p <= q else (q, p)


def smul(a, b):
    return {(p, q): sum(a[sym(p, t)] * b[sym(t, q)] for t in range(OBS)) for p, q in PAIRS}


def shift(c, a):
    return {pq: (v + c if pq[0] == pq[1] else v) for pq, v in a.items()}


def ns_weights(cov, rinv, innov, inflation, members):
    root_r = [jnp.sqrt(r) for r in rinv]
    base = (members - 1) / inflation
    b_hat = shift(base, {(p, q): cov[(p, q)] * root_r[p] * root_r[q] for p, q in PAIRS})
    norm2 = (members - OBS) * base * base
    for (p, q), v in b_hat.items():
        norm2 = norm2 + (v * v if p == q else 2.0 * (v * v))
    norm = jnp.sqrt(norm2)
    inv = 1.0 / norm
    full = (8, inv.shape[1])
    sub = lax.broadcasted_iota(jnp.int32, full, 0)

    def spread(x):
        return jnp.broadcast_to(x, full)

    state = {}
    for p, q in PAIRS:
        rest = jnp.where(sub == 1, spread(inv), jnp.where(sub == 2, 1.0, 0.0)) if p == q else jnp.zeros(full, jnp.float32)
        state[(p, q)] = jnp.where(sub == 0, spread(b_hat[(p, q)] * inv), rest)
    coef = jnp.where(sub == 1, spread(base * inv), jnp.where(sub == 3, 1.0, 0.0))
    for step in range(NS_STEPS):
        tau = 1.5 - 0.5 * spread(coef[1:2])
        t_hat = shift(1.5, {pq: -0.5 * spread(v[0:1]) for pq, v in state.items()})
        t_low = {pq: -0.5 * spread(v[1:2]) for pq, v in state.items()}
        prod = smul(state, t_hat)
        state = {pq: prod[pq] + coef * t_low[pq] for pq in PAIRS}
        coef = coef * tau
        if step < NS_STEPS - 1:
            prod = smul(state, t_hat)
            state = {pq: jnp.where(sub < 2, prod[pq] + coef * t_low[pq], state[pq]) for pq in PAIRS}
            coef = jnp.where(sub < 2, coef * tau, coef)
    inv_root = 1.0 / jnp.sqrt(norm)
    s_hat = {pq: v[2:3] * inv_root for pq, v in state.items()}
    q_mat = {pq: v[3:4] * inv_root for pq, v in state.items()}
    vec = [root_r[p] * innov[p] for p in range(OBS)]
    for _ in range(2):
        vec = [sum(s_hat[sym(p, q)] * vec[q] for q in range(OBS)) for p in range(OBS)]
    fac = math.sqrt(members - 1)
    a = fac * (coef[3:4] * inv_root)
    g = {(p, q): fac * root_r[p] * root_r[q] * q_mat[(p, q)] for p, q in PAIRS}
    e = [root_r[p] * vec[p] for p in range(OBS)]
    return a, g, e


MESH = pl.DeviceIdType.MESH
CHUNK = 256
BLK = 128
ROWS_O = 5 * BLK
PART = ROWS_O + 8
VB = 32
BF16 = jnp.bfloat16


def dot(a, b):
    return jnp.dot(a, b, preferred_element_type=jnp.float32)


def gelu_of_half(z):
    return z + z * jnp.tanh(z * (2 * 0.7978845608028654 + (8 * 0.035677408136300125) * (z * z)))


def kernel(n_dev, n_cycles, members, x_hbm, a_hbm, w_hbm, u_hbm, rinv_hbm, obs_hbm, idx_ref, infl_ref, h,
           av, wv, uv, hb, ht, mb, hid, macc, rinv_all, obs_all, part, got_sib, chip, got_chip, tot, totrow, mrow, arow, yrow,
           load_sem, rest_sem, obs_send, obs_recv, sib_send, sib_recv, chip_send, chip_recv, tot_send, tot_recv, row_send, row_recv):
    loc_members, cols, nv = h.shape
    n_layers = wv.shape[0]
    n_chunks = cols // CHUNK
    me = lax.axis_index('ens')
    core = lax.rem(me, 2)
    sib = me + 1 - 2 * core
    mate = lax.rem(me + 2, n_dev)
    obs_i = [idx_ref[p] for p in range(OBS)]

    def span(t):
        return pl.ds(pl.multiple_of(t * CHUNK, CHUNK), CHUNK)

    def load_piece(t):
        return (pltpu.make_async_copy(x_hbm.at[:, span(t), :], h.at[:, span(t), :], load_sem.at[t, 0]),
                pltpu.make_async_copy(a_hbm.at[:, span(t)], av.at[:, span(t)], load_sem.at[t, 1]))

    def start_piece(t):
        for load in load_piece(t):
            load.start()

    loads = [pltpu.make_async_copy(src, dst, rest_sem.at[i]) for i, (src, dst) in enumerate(
        ((w_hbm, wv), (u_hbm, uv), (rinv_hbm, rinv_all.at[me]), (obs_hbm, obs_all.at[me])))]
    for t in range(n_chunks):
        start_piece(t)

    barrier = pltpu.get_barrier_semaphore()
    for step in range(1, n_dev):
        pl.semaphore_signal(barrier, inc=1, device_id={'ens': lax.rem(me + step, n_dev)}, device_id_type=MESH)

    def obs_copies(step):
        dev = {'ens': lax.rem(me + step, n_dev)}
        return [pltpu.make_async_remote_copy(src_ref=ref.at[me], dst_ref=ref.at[me], send_sem=obs_send.at[step - 1, i],
                                             recv_sem=obs_recv.at[step - 1, i], device_id=dev, device_id_type=MESH)
                for i, ref in enumerate((rinv_all, obs_all))]

    def mixed(off, rows, src):
        return dot(av[pl.ds(off, rows), :], hb[src]).astype(BF16)

    def layer_rows(l, off, rows, src, put):
        for s in range(loc_members + 1):
            if s < loc_members:
                pre = dot(mb[0:rows, s * nv:(s + 1) * nv], wv[l])
            if s >= 1:
                k = s - 1
                put(k, h[k, pl.ds(off, rows), :] + dot(hid[k % 2, 0:rows, :], uv[l]))
            if s < loc_members:
                hid[s % 2, 0:rows, :] = gelu_of_half(pre).astype(BF16)

    def gather_columns(t):
        for r in range(0, cols, CHUNK):
            macc[r:r + CHUNK, :] += dot(av[r:r + CHUNK, span(t)], hb[0, span(t), :])

    def full_layer(l, c):
        src = l % 2
        if l == 0:
            for r in range(0, cols, CHUNK):
                rest = dot(av[r:r + CHUNK, cols - CHUNK:cols], hb[0, cols - CHUNK:cols, :])
                mb[r:r + CHUNK, :] = (macc[r:r + CHUNK, :] + rest).astype(BF16)
        else:
            mb[...] = mixed(0, cols, src)

        def put(k, new):
            h[k] = new
            hb[1 - src, :, k * nv:(k + 1) * nv] = new.astype(BF16)
        layer_rows(l, 0, cols, src, put)

    def last_layer(t, b):
        l = n_layers - 1
        off = pl.multiple_of(t * CHUNK + b * BLK, BLK)
        mb[0:BLK, :] = mixed(off, BLK, l % 2)

        def put(k, new):
            ht[t, b, k * nv:(k + 1) * nv, :] = new.T
        layer_rows(l, off, BLK, l % 2, put)

    def stats(c, t, b):
        ho = [[ht[t, b, pl.ds(k * nv + obs_i[p], 1), :] for k in range(loc_members)] for p in range(OBS)]
        mo = [sum(x[1:], x[0]) * (1.0 / loc_members) for x in ho]
        y = [[x - mo[p] for x in ho[p]] for p in range(OBS)]
        for p in range(OBS):
            part[c, t, b, ROWS_O + p:ROWS_O + p + 1, :] = mo[p]
        for v in range(0, nv, VB):
            x = [ht[t, b, k * nv + v:k * nv + v + VB, :] for k in range(loc_members)]
            m = sum(x[1:], x[0]) * (1.0 / loc_members)
            d = [z - m for z in x]
            part[c, t, b, v:v + VB, :] = m
            for p in range(OBS):
                o = (p + 1) * BLK + v
                part[c, t, b, o:o + VB, :] = sum(y[p][k] * d[k] for k in range(loc_members))

    def merge(dst, dst_o, one, two, two_o, half_n, keep):
        for p in range(OBS):
            dst_o[p:p + 1, :] = 0.5 * (one[ROWS_O + p:ROWS_O + p + 1, :] + two_o[p])
        sc = [half_n * (two_o[p] - one[ROWS_O + p:ROWS_O + p + 1, :]) for p in range(OBS)]
        for v in range(0, nv, VB):
            ma, mbb = one[v:v + VB, :], two[v:v + VB, :]
            dst[v:v + VB, :] = 0.5 * (ma + mbb)
            dm = mbb - ma
            for p in range(OBS):
                o = (p + 1) * BLK + v
                val = one[o:o + VB, :] + two[o:o + VB, :] + sc[p] * dm
                dst[o:o + VB, :] = val
                if keep:
                    arow[o - BLK:o - BLK + VB, :] = val
    def sib_copy(c, t):
        return pltpu.make_async_remote_copy(
            src_ref=part.at[c, t, 1 - core], dst_ref=got_sib.at[c, t], send_sem=sib_send.at[c, t], recv_sem=sib_recv.at[c, t],
            device_id={'ens': sib}, device_id_type=MESH)

    def chip_copy(c, t):
        return pltpu.make_async_remote_copy(
            src_ref=chip.at[c, t, 0:ROWS_O], dst_ref=got_chip.at[c, t], send_sem=chip_send.at[c, t], recv_sem=chip_recv.at[c, t],
            device_id={'ens': mate}, device_id_type=MESH)

    def tot_copy(c, t):
        return pltpu.make_async_remote_copy(
            src_ref=tot.at[c, t, core], dst_ref=tot.at[c, t, core], send_sem=tot_send.at[c, t], recv_sem=tot_recv.at[c, t],
            device_id={'ens': sib}, device_id_type=MESH)

    def row_copy(c, t):
        return pltpu.make_async_remote_copy(
            src_ref=totrow.at[c, t, core], dst_ref=totrow.at[c, t, core], send_sem=row_send.at[c, t], recv_sem=row_recv.at[c, t],
            device_id={'ens': sib}, device_id_type=MESH)

    def first_merge(c, t):
        sib_copy(c, t).wait_recv()
        two = got_sib.at[c, t]
        two_o = [two[ROWS_O + p:ROWS_O + p + 1, :] for p in range(OBS)]
        merge(chip.at[c, t], chip.at[c, t, ROWS_O:PART], part.at[c, t, core], two, two_o, loc_members / 2, False)
        chip_copy(c, t).start()

    def second_merge(c, t):
        chip_copy(c, t).wait_recv()
        two = got_chip.at[c, t]
        mrow[...] = two[0:BLK, :]
        two_o = [mrow[pl.ds(obs_i[p], 1), :] for p in range(OBS)]
        merge(tot.at[c, t, core], totrow.at[c, t, core], chip.at[c, t], two, two_o, loc_members, True)
        for n, (p, q) in enumerate(PAIRS):
            totrow[c, t, core, OBS + n:OBS + n + 1, :] = arow[pl.ds(p * BLK + obs_i[q], 1), :]
        row_copy(c, t).start()
        tot_copy(c, t).start()

    def weights(c, t, b):
        lanes = pl.ds(pl.multiple_of(b * BLK, BLK), BLK)

        def row(r):
            return totrow[c, t, b, r:r + 1, :]

        cov = {pq: row(OBS + n) for n, pq in enumerate(PAIRS)}
        rinv = [rinv_all[t, p:p + 1, lanes] for p in range(OBS)]
        innov = [obs_all[t, c, p:p + 1, lanes] - row(p) for p in range(OBS)]
        for k in range(loc_members):
            for p in range(OBS):
                yrow[k * OBS + p] = ht[t, b, pl.ds(k * nv + obs_i[p], 1), :] - row(p)
        return ns_weights(cov, rinv, innov, infl_ref[0], members)

    def apply(c, t, b, ca, cg, ce):
        rows = pl.ds(pl.multiple_of(t * CHUNK + b * BLK, BLK), BLK)
        for v in range(0, nv, VB):
            m = tot[c, t, b, v:v + VB, :]
            mom = [tot[c, t, b, (p + 1) * BLK + v:(p + 1) * BLK + v + VB, :] for p in range(OBS)]
            base = m + sum(ce[p] * mom[p] for p in range(OBS))
            mix = [sum(cg[sym(p, q)] * mom[q] for q in range(OBS)) for p in range(OBS)]
            for k in range(loc_members):
                r = k * nv + v
                new = base + ca * (ht[t, b, r:r + VB, :] - m)
                for p in range(OBS):
                    new = new + yrow[k * OBS + p] * mix[p]
                ht[t, b, r:r + VB, :] = new
        for k in range(loc_members):
            blk = ht[t, b, k * nv:(k + 1) * nv, :].T
            h[k, rows, :] = blk
            if c < n_cycles - 1:
                hb[0, rows, k * nv:(k + 1) * nv] = blk.astype(BF16)

    def enter(t):
        for load in load_piece(t):
            load.wait()
        for k in range(loc_members):
            hb[0, span(t), k * nv:(k + 1) * nv] = h[k, span(t), :].astype(BF16)

    macc[...] = jnp.zeros_like(macc)

    def begin(t, _):
        enter(t)

        @pl.when(t == 0)
        def _():
            for load in loads:
                load.start()
        gather_columns(t)
        return 0
    lax.fori_loop(0, n_chunks - 1, begin, 0)
    enter(n_chunks - 1)
    loads[0].wait()
    wv[...] = wv[...] * jnp.bfloat16(0.5)
    loads[1].wait()

    for c in range(n_cycles):
        for l in range(n_layers - 1):
            full_layer(l, c)
            if c == 0 and l == 0:
                for load in loads[2:]:
                    load.wait()
                pl.semaphore_wait(barrier, n_dev - 1)
                for step in range(1, n_dev):
                    for copy in obs_copies(step):
                        copy.start()

        def last(t, _, c=c):
            last_layer(t, 1 - core)
            stats(c, t, 1 - core)
            sib_copy(c, t).start()
            last_layer(t, core)
            stats(c, t, core)
            first_merge(c, t)
            return 0
        lax.fori_loop(0, n_chunks, last, 0)

        if c == 0:
            for step in range(1, n_dev):
                for copy in obs_copies(step):
                    copy.wait()
        if c < n_cycles - 1:
            macc[...] = jnp.zeros_like(macc)

        def finish(t, _, c=c):
            sib_copy(c, t).wait_send()
            second_merge(c, t)
            apply(c, t, core, *weights(c, t, core))
            chip_copy(c, t).wait_send()
            row_copy(c, t).wait_recv()
            other = weights(c, t, 1 - core)
            tot_copy(c, t).wait_recv()
            apply(c, t, 1 - core, *other)
            if c < n_cycles - 1:
                pl.when(t < n_chunks - 1)(lambda: gather_columns(t))
            tot_copy(c, t).wait_send()
            row_copy(c, t).wait_send()
            return 0
        lax.fori_loop(0, n_chunks, finish, 0)


def solution(mesh):
    n_dev = mesh.shape['ens']

    def per_device(x_loc, col_mix, w_in, w_out, obs_loc, rinv_loc, obs_idx, inflation):
        loc, cols, nv = x_loc.shape
        layers, _, ff = w_in.shape
        cycles = obs_loc.shape[0]
        n_chunks = cols // CHUNK
        rinv_t = rinv_loc.T
        obs_t = jnp.swapaxes(obs_loc, 1, 2)
        vm = pl.BlockSpec(memory_space=pltpu.VMEM)
        sm = pl.BlockSpec(memory_space=pltpu.SMEM)
        dma = pltpu.SemaphoreType.DMA
        f32 = jnp.float32
        return pl.pallas_call(
            functools.partial(kernel, n_dev, cycles, loc * n_dev),
            out_shape=pltpu.VMEM(x_loc.shape, x_loc.dtype),
            in_specs=[pl.BlockSpec(memory_space=pltpu.HBM)] * 6 + [sm] * 2,
            out_specs=vm,
            scratch_shapes=[
                pltpu.VMEM((cols, cols), BF16),
                pltpu.VMEM((layers, nv, ff), BF16),
                pltpu.VMEM((layers, ff, nv), BF16),
                pltpu.VMEM((2, cols, loc * nv), BF16),
                pltpu.VMEM((n_chunks, 2, loc * nv, BLK), f32),
                pltpu.VMEM((cols, loc * nv), BF16),
                pltpu.VMEM((2, cols, ff), BF16),
                pltpu.VMEM((cols, loc * nv), f32),
                pltpu.VMEM((n_dev,) + rinv_t.shape, f32),
                pltpu.VMEM((n_dev,) + obs_t.shape, f32),
                pltpu.VMEM((cycles, n_chunks, 2, PART, BLK), f32),
                pltpu.VMEM((cycles, n_chunks, PART, BLK), f32),
                pltpu.VMEM((cycles, n_chunks, PART, BLK), f32),
                pltpu.VMEM((cycles, n_chunks, ROWS_O, BLK), f32),
                pltpu.VMEM((cycles, n_chunks, 2, ROWS_O, BLK), f32),
                pltpu.VMEM((cycles, n_chunks, 2, 16, BLK), f32),
                pltpu.VMEM((BLK, BLK), f32),
                pltpu.VMEM((OBS * BLK, BLK), f32),
                pltpu.VMEM((loc * OBS, 1, BLK), f32),
                dma((n_chunks, 2)), dma((4,)),
                dma((n_dev - 1, 2)), dma((n_dev - 1, 2)),
                dma((cycles, n_chunks)), dma((cycles, n_chunks)),
                dma((cycles, n_chunks)), dma((cycles, n_chunks)),
                dma((cycles, n_chunks)), dma((cycles, n_chunks)),
                dma((cycles, n_chunks)), dma((cycles, n_chunks)),
            ],
            compiler_params=pltpu.CompilerParams(collective_id=0, has_side_effects=True, vmem_limit_bytes=58 * 1024 * 1024),
        )(x_loc, col_mix, w_in, w_out, rinv_t, obs_t, obs_idx, inflation)

    state_spec = P(('case', 'ens'), None, None)
    in_specs = (state_spec, P(), P(), P(), P(None, ('case', 'ens'), None), P(('case', 'ens'), None), P(), P())
    return jax.shard_map(per_device, mesh=mesh, in_specs=in_specs, out_specs=state_spec, check_vma=False)
```
